64 devices in a mesh: dp: 4 (over x, y), cp: 16 (over z, core).
Axes of the slice: x: 2, y: 2, z: 8, core: 2. Of those that a mesh axis runs over, the one named last changes fastest.
The devices are a block of a 4x4x8 slice.
Arguments:
- latents: bfloat16 [8, 128, 128, 4], P('dp', 'cp'), parts along dimension 0
- w_in: bfloat16 [3, 3, 4, 512], replicated
- b_in: bfloat16 [512], replicated
- w_conv: bfloat16 [4, 3, 3, 512, 512], replicated
- b_conv: bfloat16 [4, 512], replicated
- gn_scale: bfloat16 [5, 512], replicated
- gn_shift: bfloat16 [5, 512], replicated
- w_attn: bfloat16 [4, 512, 512], replicated
- b_attn: bfloat16 [4, 512], replicated
Outputs:
- output: bfloat16 [8, 128, 128, 512], P('dp', 'cp'), parts along dimension 0
There are 4 independent parts. The reference program is written for one: setup_inputs(seed, part) draws one part's arguments, and reference() takes and returns one part's arrays. A program takes and returns all parts, laid end to end along the dimension named above; an argument that names none is the same for every part.
All inputs are finite; a program needn't handle non-finite values.
Results may differ from the reference program's by a relative error of at most 0.02.
Values are sent between devices in bfloat16 or wider.
A program may use at most 768 MiB of HBM per device.

```python
import jax
import jax.numpy as jnp
from jax import lax

SAMPLES = 2
LAT_H = 128
LAT_W = 128
Z_CH = 4
CHANNELS = 512
GROUPS = 32
QUERY_TOKENS = 1024
GN_EPS = 1e-6


def setup_inputs(seed: int = 0, part: int = 0) -> dict:
    root_key = jax.random.key(seed)
    rand_keys = jax.random.split(root_key, 9)
    lat_keys = jax.random.split(jax.random.fold_in(rand_keys[0], part), 4)
    lat_noise = jax.random.normal(lat_keys[0], (SAMPLES, LAT_H, LAT_W, Z_CH), jnp.float32)
    row_pos = (2.0 * jnp.arange(LAT_H, dtype=jnp.float32) / (LAT_H - 1) - 1.0).reshape(1, LAT_H, 1, 1)
    row_slope = 0.8 * jax.random.normal(lat_keys[1], (SAMPLES, 1, 1, Z_CH), jnp.float32)
    row_scale = jax.random.uniform(lat_keys[2], (SAMPLES, LAT_H, 1, 1), jnp.float32, 0.6, 1.4)
    row_shift = 0.3 * jax.random.normal(lat_keys[3], (SAMPLES, LAT_H, 1, Z_CH), jnp.float32)
    latents = lat_noise * row_scale + row_slope * row_pos + row_shift
    attn_gain = jnp.array([2.4, 2.4, 1.0, 1.0], dtype=jnp.float32).reshape(4, 1, 1)
    w_in = jax.random.normal(rand_keys[1], (3, 3, Z_CH, CHANNELS), jnp.float32) * (9 * Z_CH) ** -0.5
    b_in = 0.5 * jax.random.normal(rand_keys[2], (CHANNELS,), jnp.float32)
    w_conv = jax.random.normal(rand_keys[3], (4, 3, 3, CHANNELS, CHANNELS), jnp.float32) * (9 * CHANNELS) ** -0.5
    b_conv = 0.3 * jax.random.normal(rand_keys[4], (4, CHANNELS), jnp.float32)
    gn_scale = 1.0 + 0.3 * jax.random.normal(rand_keys[5], (5, CHANNELS), jnp.float32)
    gn_shift = 0.3 * jax.random.normal(rand_keys[6], (5, CHANNELS), jnp.float32)
    w_attn = jax.random.normal(rand_keys[7], (4, CHANNELS, CHANNELS), jnp.float32) * attn_gain * CHANNELS ** -0.5
    b_attn = 0.3 * jax.random.normal(rand_keys[8], (4, CHANNELS), jnp.float32)
    return {
        'latents': latents.astype(jnp.bfloat16),
        'w_in': w_in.astype(jnp.bfloat16),
        'b_in': b_in.astype(jnp.bfloat16),
        'w_conv': w_conv.astype(jnp.bfloat16),
        'b_conv': b_conv.astype(jnp.bfloat16),
        'gn_scale': gn_scale.astype(jnp.bfloat16),
        'gn_shift': gn_shift.astype(jnp.bfloat16),
        'w_attn': w_attn.astype(jnp.bfloat16),
        'b_attn': b_attn.astype(jnp.bfloat16),
    }


def conv3x3(x_val, weight, conv_bias):
    conv_out = lax.conv_general_dilated(x_val.astype(jnp.float32), weight.astype(jnp.float32), (1, 1), 'SAME', dimension_numbers=('NHWC', 'HWIO', 'NHWC'))
    return conv_out + conv_bias.astype(jnp.float32)


def group_norm(x_val, norm_gain, norm_bias):
    n_batch, n_rows, n_width, n_chan = x_val.shape
    grouped = x_val.astype(jnp.float32).reshape(n_batch, n_rows, n_width, GROUPS, n_chan // GROUPS)
    grp_mean = jnp.mean(grouped, axis=(1, 2, 4), keepdims=True)
    centered = grouped - grp_mean
    grp_var = jnp.mean(jnp.square(centered), axis=(1, 2, 4), keepdims=True)
    normed = (centered * lax.rsqrt(grp_var + GN_EPS)).reshape(x_val.shape)
    return normed * norm_gain.astype(jnp.float32) + norm_bias.astype(jnp.float32)


def resnet_block(h_val, w_conv, b_conv, gn_scale, gn_shift, conv_idx, norm_idx):
    act_in = jax.nn.silu(group_norm(h_val, gn_scale[norm_idx], gn_shift[norm_idx])).astype(jnp.bfloat16)
    mid_act = conv3x3(act_in, w_conv[conv_idx], b_conv[conv_idx]).astype(jnp.bfloat16)
    act_two = jax.nn.silu(group_norm(mid_act, gn_scale[norm_idx + 1], gn_shift[norm_idx + 1])).astype(jnp.bfloat16)
    conv_two = conv3x3(act_two, w_conv[conv_idx + 1], b_conv[conv_idx + 1])
    return (h_val.astype(jnp.float32) + conv_two).astype(jnp.bfloat16)


def attention(h_val, w_attn, b_attn, norm_gain, norm_bias):
    n_batch, n_rows, n_width, n_chan = h_val.shape
    normed = group_norm(h_val, norm_gain, norm_bias).astype(jnp.bfloat16).reshape(-1, n_chan)

    def project(j_idx):
        proj = jnp.dot(normed, w_attn[j_idx], preferred_element_type=jnp.float32) + b_attn[j_idx].astype(jnp.float32)
        return proj.astype(jnp.bfloat16).reshape(n_batch, n_rows * n_width, n_chan)

    queries = project(0)
    keys_all = project(1)
    vals_all = project(2)
    block_rows = max([divisor for divisor in range(1, n_rows + 1) if n_rows % divisor == 0 and divisor * n_width <= QUERY_TOKENS] + [1])
    n_blocks = n_rows // block_rows
    att_scale = n_chan ** -0.5

    def one_sample(operands):
        q_sample, k_sample, v_sample = operands

        def one_block(q_block):
            scores = jnp.dot(q_block, k_sample.T, preferred_element_type=jnp.float32) * att_scale
            attn_prob = jax.nn.softmax(scores, axis=-1).astype(jnp.bfloat16)
            return jnp.dot(attn_prob, v_sample, preferred_element_type=jnp.float32).astype(jnp.bfloat16)

        return lax.map(one_block, q_sample.reshape(n_blocks, block_rows * n_width, n_chan))

    attended = lax.map(one_sample, (queries, keys_all, vals_all)).reshape(-1, n_chan)
    proj_out = jnp.dot(attended, w_attn[3], preferred_element_type=jnp.float32) + b_attn[3].astype(jnp.float32)
    return (h_val.astype(jnp.float32) + proj_out.reshape(h_val.shape)).astype(jnp.bfloat16)


def reference(latents, w_in, b_in, w_conv, b_conv, gn_scale, gn_shift, w_attn, b_attn):
    hidden = conv3x3(latents, w_in, b_in).astype(jnp.bfloat16)
    hidden = resnet_block(hidden, w_conv, b_conv, gn_scale, gn_shift, 0, 0)
    hidden = attention(hidden, w_attn, b_attn, gn_scale[2], gn_shift[2])
    hidden = resnet_block(hidden, w_conv, b_conv, gn_scale, gn_shift, 2, 3)
    return hidden
```

```python
import functools
import math

import jax
import jax.numpy as jnp
from jax import lax
from jax.experimental import pallas as pl
from jax.experimental.pallas import tpu as pltpu
from jax.sharding import PartitionSpec as P

F32 = jnp.float32
BF16 = jnp.bfloat16
GROUPS = 32
GN_EPS = 1e-6
MESH = pl.DeviceIdType.MESH
B_IN, B_CONV, GAIN, SHIFT, B_ATT, N_PAR = 0, 1, 5, 10, 15, 24


def group_total(x_val, steps):
    lane = lax.broadcasted_iota(jnp.int32, x_val.shape, 1)
    width = x_val.shape[1]
    for step in steps:
        above = pltpu.roll(x_val, width - step, 1)
        below = pltpu.roll(x_val, step, 1)
        x_val = x_val + jnp.where((lane & step) == 0, above, below)
    return x_val


def body(cfg, zcol, w_in, par, bk_col, w_conv, w_att, out, hbuf, tbuf, u3, wbuf, wabuf, halo, stat_src, stat_rcv,
         ring, qbuf, acc, mx, ls, nbuf, kt, vbuf, obuf, osend,
         w_sem, wa_sem, st_send, st_recv, ha_send, ha_recv, rg_send, rg_recv, sw_send, sw_recv, o_send, o_recv, out_sem):
    n_dev, n_rows, width, n_chan = cfg
    n_tok = n_rows * width
    lanes = n_chan // GROUPS
    n_vreg = n_chan // 128
    count = n_dev * n_tok * lanes
    me = lax.axis_index('cp')
    core = lax.rem(me, 2)
    mate = me + 1 - 2 * core
    ahead = lax.rem(me + 2, n_dev)
    behind = lax.rem(me + n_dev - 2, n_dev)
    below = lax.rem(me + 1, n_dev)
    above = lax.rem(me + n_dev - 1, n_dev)

    barrier = pltpu.get_barrier_semaphore()
    for dist in range(1, n_dev):
        pl.semaphore_signal(barrier, inc=1, device_id={'cp': lax.rem(me + dist, n_dev)}, device_id_type=MESH)

    def load_weights(idx):
        return pltpu.make_async_copy(w_conv.at[idx], wbuf.at[idx % 2], w_sem.at[idx % 2])

    load_weights(0).start()
    load_weights(1).start()
    load_att = pltpu.make_async_copy(w_att, wabuf, wa_sem)
    load_att.start()

    def row_of(idx):
        return par[pl.ds(idx, 1), :]

    def remote(src, dst, send_sem, recv_sem, dev):
        return pltpu.make_async_remote_copy(src_ref=src, dst_ref=dst, send_sem=send_sem, recv_sem=recv_sem,
                                            device_id={'cp': dev}, device_id_type=MESH)

    def partial(val):
        parts = val.reshape(val.shape[0] // 8, 8, n_chan)
        return jnp.sum(parts, axis=0), jnp.sum(parts * parts, axis=0)

    def send_stats(exch, smp, sums):
        row = lax.broadcasted_iota(jnp.int32, (8, n_chan), 0)
        first = jnp.sum(sums[0], axis=0, keepdims=True)
        second = jnp.sum(sums[1], axis=0, keepdims=True)
        both = jnp.where(row == 0, first, jnp.where(row == 1, second, 0.0))
        both = group_total(both, (1, 2, 4, 8))
        lane = lax.broadcasted_iota(jnp.int32, (8, 128), 1)
        packed = both[:, :128]
        for idx in range(1, n_vreg):
            packed = jnp.where((lane & 3) == idx, both[:, idx * 128:(idx + 1) * 128], packed)
        stat_src[exch, smp] = packed
        for dist in range(1, n_dev):
            remote(stat_src.at[exch, smp], stat_rcv.at[exch, smp, dist - 1], st_send.at[exch, smp],
                   st_recv.at[exch, smp], lax.rem(me + dist, n_dev)).start()

    def wait_stats(exch, smp):
        every = stat_rcv.at[exch, smp]
        pltpu.make_async_copy(every, every, st_recv.at[exch, smp]).wait()
        pltpu.make_async_copy(every, every, st_send.at[exch, smp]).wait()

    def affine(exch, smp, norm):
        total = stat_src[exch, smp] + jnp.sum(stat_rcv[exch, smp], axis=0)
        lane = lax.broadcasted_iota(jnp.int32, (8, 128), 1)
        spread = [group_total(jnp.where((lane & 3) == idx, total, 0.0), (1, 2)) for idx in range(n_vreg)]
        full = jnp.concatenate(spread, axis=1)
        mean = full[0:1, :] / count
        inv = lax.rsqrt(full[1:2, :] / count - mean * mean + GN_EPS)
        mul = inv * row_of(GAIN + norm)
        return mul, row_of(SHIFT + norm) - mean * mul

    def halo_copies(exch, smp, buf):
        top = remote(buf.at[smp, pl.ds(0, width)], halo.at[exch, smp, 1], ha_send.at[exch, smp, 0], ha_recv.at[exch, smp, 1], above)
        bottom = remote(buf.at[smp, pl.ds(n_tok - width, width)], halo.at[exch, smp, 0], ha_send.at[exch, smp, 1], ha_recv.at[exch, smp, 0], below)
        return top, bottom

    def send_halo(exch, smp, buf):
        for copy in halo_copies(exch, smp, buf):
            copy.start()

    def wait_halo(exch, smp, buf):
        for copy in halo_copies(exch, smp, buf):
            copy.wait()

    def conv_sample(smp, conv, norm, exch, hexch, src, dst, res):
        wait_stats(exch, smp)
        wait_halo(hexch, smp, src)
        mul, add = affine(exch, smp, norm)
        col = lax.broadcasted_iota(jnp.int32, (width, n_chan), 0)

        def put(row, x_val, keep):
            y_val = x_val.astype(F32) * mul + add
            half = 0.5 * y_val
            act = half + half * jnp.tanh(half)
            if keep is not None:
                act = jnp.where(keep, act, 0.0)
            left = jnp.where(col == 0, 0.0, pltpu.roll(act, 1, 0))
            right = jnp.where(col == width - 1, 0.0, pltpu.roll(act, width - 1, 0))
            u3[pl.ds(row * width, width), :n_chan] = left.astype(BF16)
            u3[pl.ds(row * width, width), n_chan:2 * n_chan] = act.astype(BF16)
            u3[pl.ds(row * width, width), 2 * n_chan:] = right.astype(BF16)

        put(0, halo[hexch, smp, 0], me > 0)
        put(n_rows + 1, halo[hexch, smp, 1], me < n_dev - 1)

        def put_row(row, carry):
            put(row + 1, src[smp, pl.ds(row * width, width), :], None)
            return carry

        lax.fori_loop(0, n_rows, put_row, 0)
        span = n_tok // 2
        bias = row_of(B_CONV + conv)
        taps = 3 * n_chan

        def block(idx, sums):
            base = idx * span
            total = bias
            for dy in range(3):
                total = total + jnp.dot(u3[pl.ds(base + dy * width, span), :], wbuf[conv % 2, dy * taps:(dy + 1) * taps, :],
                                        preferred_element_type=F32)
            if res is not None:
                total = total + res[smp, pl.ds(base, span), :].astype(F32)
            rounded = total.astype(BF16)
            dst[smp, pl.ds(base, span), :] = rounded
            one, two = partial(rounded.astype(F32))
            return sums[0] + one, sums[1] + two

        zero = jnp.zeros((8, n_chan), F32)
        return lax.fori_loop(0, 2, block, (zero, zero))

    def first(smp, carry):
        total = jnp.dot(zcol[smp], w_in[...], preferred_element_type=F32) + row_of(B_IN)
        rounded = total.astype(BF16)
        hbuf[smp] = rounded

        @pl.when(smp == 0)
        def _():
            pl.semaphore_wait(barrier, n_dev - 1)

        send_halo(0, smp, hbuf)
        send_stats(0, smp, partial(rounded.astype(F32)))
        return carry

    lax.fori_loop(0, 2, first, 0)

    load_weights(0).wait()

    def stage0(smp, carry):
        sums = conv_sample(smp, 0, 0, 0, 0, hbuf, tbuf, None)
        send_halo(1, smp, tbuf)
        send_stats(1, smp, sums)
        return carry

    lax.fori_loop(0, 2, stage0, 0)
    load_weights(2).start()
    load_weights(1).wait()

    def forward(idx):
        return remote(ring.at[idx], ring.at[idx + 2], rg_send.at[0, idx], rg_recv.at[idx + 2], ahead)

    def backward(idx):
        src = 1 - idx if isinstance(idx, int) and idx < 2 else idx + 7
        return remote(ring.at[src], ring.at[idx + 9], rg_send.at[1, idx], rg_recv.at[idx + 9], behind)

    def swap():
        return remote(hbuf.at[1 - core], ring.at[1], sw_send, sw_recv, mate)

    def stage1(smp, carry):
        sums = conv_sample(smp, 1, 1, 1, 1, tbuf, hbuf, hbuf)
        send_stats(2, smp, sums)

        @pl.when(smp == 1 - core)
        def _():
            swap().start()

        @pl.when(smp == core)
        def _():
            ring[0] = hbuf[smp]
            forward(0).start()

        return carry

    lax.fori_loop(0, 2, stage1, 0)
    load_weights(3).start()
    backward(1).start()
    swap().wait()
    forward(1).start()
    backward(0).start()
    load_att.wait()

    wait_stats(2, core)
    wait_stats(2, 1 - core)
    mul2, add2 = affine(2, core, 2)
    scale = n_chan ** -0.5 * math.log2(math.e)
    mx[...] = jnp.full(mx.shape, -jnp.inf, F32)
    ls[...] = jnp.zeros(ls.shape, F32)
    acc[...] = jnp.zeros(acc.shape, F32)

    def norm_slot(slot):
        nbuf[...] = (ring[slot].astype(F32) * mul2 + add2).astype(BF16)

    def query(slot, carry):
        norm_slot(slot)
        proj = jnp.dot(nbuf[...], wabuf[0], preferred_element_type=F32) + row_of(B_ATT)
        qbuf[pl.ds(slot * n_tok, n_tok), :] = proj.astype(BF16)
        return carry

    lax.fori_loop(0, 2, query, 0)
    q_len = n_tok // 2

    def attend(slot):
        norm_slot(slot)
        keys = lax.dot_general(wabuf[1], nbuf[...], (((1,), (1,)), ((), ())), preferred_element_type=F32)
        kt[...] = (keys + bk_col[:, 0:1]).astype(BF16)
        vals = jnp.dot(nbuf[...], wabuf[2], preferred_element_type=F32) + row_of(B_ATT + 2)
        vbuf[...] = vals.astype(BF16)

        def one(blk, carry):
            rows = pl.ds(blk * q_len, q_len)
            scores = jnp.dot(qbuf[rows, :], kt[...], preferred_element_type=F32)
            old = mx[rows, :]
            new = jnp.maximum(old, jnp.max(scores, axis=1, keepdims=True) * scale)
            fade = jnp.exp2(old - new)
            prob = jnp.exp2(scores * scale - new[:, 0:1])
            mx[rows, :] = new
            ls[rows, :] = ls[rows, :] * fade + jnp.sum(prob, axis=1, keepdims=True)
            acc[rows, :] = acc[rows, :] * fade[:, 0:1] + jnp.dot(prob.astype(BF16), vbuf[...], preferred_element_type=F32)
            return carry

        lax.fori_loop(0, 4, one, 0)

    def own(slot, carry):
        attend(slot)
        return carry

    lax.fori_loop(0, 2, own, 0)

    def step(idx, carry):
        forward(idx - 1).wait_recv()

        @pl.when(idx <= 5)
        def _():
            forward(idx + 1).start()

        remote(ring.at[idx + 8], ring.at[idx + 8], rg_send.at[1, idx - 1], rg_recv.at[idx + 8], behind).wait_recv()

        @pl.when(idx <= 5)
        def _():
            backward(idx + 1).start()

        def both(side, inner):
            attend(idx + 1 + 7 * side)
            return inner

        return lax.fori_loop(0, 2, both, carry)

    lax.fori_loop(1, 8, step, 0)

    def drain(idx, carry):
        forward(idx).wait_send()
        remote(ring.at[0], ring.at[9], rg_send.at[1, idx], rg_recv.at[9], behind).wait_send()
        return carry

    lax.fori_loop(0, 7, drain, 0)

    osend[...] = (acc[n_tok:, :] / ls[n_tok:, 0:1]).astype(BF16)
    give = remote(osend, obuf.at[1], o_send, o_recv, mate)
    give.start()
    obuf[0] = (acc[:n_tok, :] / ls[:n_tok, 0:1]).astype(BF16)

    def project(side, carry):
        @pl.when(side == 1)
        def _():
            give.wait()

        smp = lax.rem(core + side, 2)
        total = jnp.dot(obuf[side], wabuf[3], preferred_element_type=F32) + row_of(B_ATT + 3)
        rounded = (hbuf[smp].astype(F32) + total).astype(BF16)
        hbuf[smp] = rounded
        send_halo(2, smp, hbuf)
        send_stats(3, smp, partial(rounded.astype(F32)))
        return carry

    lax.fori_loop(0, 2, project, 0)
    load_weights(2).wait()

    def stage2(smp, carry):
        sums = conv_sample(smp, 2, 3, 3, 2, hbuf, tbuf, None)
        send_halo(3, smp, tbuf)
        send_stats(4, smp, sums)
        return carry

    lax.fori_loop(0, 2, stage2, 0)
    load_weights(3).wait()

    def write(smp):
        return pltpu.make_async_copy(tbuf.at[smp], out.at[smp], out_sem.at[smp])

    def stage3(smp, carry):
        conv_sample(smp, 3, 4, 4, 3, tbuf, tbuf, hbuf)
        write(smp).start()
        return carry

    lax.fori_loop(0, 2, stage3, 0)
    write(0).wait()
    write(1).wait()


def decoder(n_dev, zcol, w_in, par, bk_col, w_conv, w_att, n_rows, width):
    n_chan = w_in.shape[1]
    n_tok = n_rows * width
    vmem = pltpu.VMEM
    dma = pltpu.SemaphoreType.DMA
    in_vmem = pl.BlockSpec(memory_space=pltpu.VMEM)
    in_any = pl.BlockSpec(memory_space=pl.ANY)
    scratch = [
        vmem((2, n_tok, n_chan), BF16),
        vmem((2, n_tok, n_chan), BF16),
        vmem((n_tok + 2 * width, 3 * n_chan), BF16),
        vmem((2, 9 * n_chan, n_chan), BF16),
        vmem((4, n_chan, n_chan), BF16),
        vmem((4, 2, 2, width, n_chan), BF16),
        vmem((5, 2, 8, 128), F32),
        vmem((5, 2, n_dev - 1, 8, 128), F32),
        vmem((n_dev, n_tok, n_chan), BF16),
        vmem((2 * n_tok, n_chan), BF16),
        vmem((2 * n_tok, n_chan), F32),
        vmem((2 * n_tok, 128), F32),
        vmem((2 * n_tok, 128), F32),
        vmem((n_tok, n_chan), BF16),
        vmem((n_chan, n_tok), BF16),
        vmem((n_tok, n_chan), BF16),
        vmem((2, n_tok, n_chan), BF16),
        vmem((n_tok, n_chan), BF16),
        dma((2,)), dma, dma((5, 2)), dma((5, 2)), dma((4, 2, 2)), dma((4, 2, 2)), dma((2, 7)), dma((16,)),
        dma, dma, dma, dma, dma((2,)),
    ]
    return pl.pallas_call(
        functools.partial(body, (n_dev, n_rows, width, n_chan)),
        out_shape=jax.ShapeDtypeStruct((2, n_tok, n_chan), BF16),
        in_specs=[in_vmem, in_vmem, in_vmem, in_vmem, in_any, in_any],
        out_specs=in_any,
        scratch_shapes=scratch,
        compiler_params=pltpu.CompilerParams(collective_id=0, has_side_effects=True, vmem_limit_bytes=67043328),
    )(zcol, w_in, par, bk_col, w_conv, w_att)


def solution(mesh):
    n_dev = mesh.shape['cp']

    def local_fn(latents, w_in, b_in, w_conv, b_conv, gn_scale, gn_shift, w_attn, b_attn):
        n_batch, n_rows, width, n_z = latents.shape
        n_chan = w_in.shape[-1]
        down_pairs = [(sender, sender + 1) for sender in range(n_dev - 1)]
        up_pairs = [(sender + 1, sender) for sender in range(n_dev - 1)]
        from_above = lax.ppermute(latents[:, -1:], 'cp', down_pairs)
        from_below = lax.ppermute(latents[:, :1], 'cp', up_pairs)
        padded = jnp.concatenate([from_above, latents, from_below], axis=1)
        padded = jnp.pad(padded, ((0, 0), (0, 0), (1, 1), (0, 0)))
        taps = [padded[:, dy:dy + n_rows, dx:dx + width] for dy in range(3) for dx in range(3)]
        taps.append(jnp.zeros((n_batch, n_rows, width, 128 - 9 * n_z), BF16))
        zcol = jnp.concatenate(taps, axis=-1).reshape(n_batch, n_rows * width, 128)
        w_first = jnp.pad(w_in.reshape(9 * n_z, n_chan), ((0, 128 - 9 * n_z), (0, 0)))
        par = jnp.concatenate([b_in[None], b_conv, gn_scale, gn_shift, b_attn]).astype(F32)
        par = jnp.pad(par, ((0, N_PAR - par.shape[0]), (0, 0)))
        bk_col = jnp.broadcast_to(b_attn[1].astype(F32)[:, None], (n_chan, 128))
        w_att = jnp.stack([w_attn[0], w_attn[1].T, w_attn[2], w_attn[3]])
        out = decoder(n_dev, zcol, w_first, par, bk_col, w_conv.reshape(4, 9 * n_chan, n_chan), w_att, n_rows, width)
        return out.reshape(n_batch, n_rows, width, n_chan)

    band_spec = P('dp', 'cp')
    whole_spec = P()
    return jax.shard_map(local_fn, mesh=mesh, in_specs=(band_spec,) + (whole_spec,) * 8, out_specs=band_spec, check_vma=False)
```

```python
import functools
import math

import jax
import jax.numpy as jnp
from jax import lax
from jax.experimental import pallas as pl
from jax.experimental.pallas import tpu as pltpu
from jax.sharding import PartitionSpec as P

F32 = jnp.float32
BF16 = jnp.bfloat16
GROUPS = 32
GN_EPS = 1e-6
MESH = pl.DeviceIdType.MESH
B_IN, B_CONV, GAIN, SHIFT, B_ATT, N_PAR = 0, 1, 5, 10, 15, 24


def group_total(x_val, steps):
    lane = lax.broadcasted_iota(jnp.int32, x_val.shape, 1)
    width = x_val.shape[1]
    for step in steps:
        above = pltpu.roll(x_val, width - step, 1)
        below = pltpu.roll(x_val, step, 1)
        x_val = x_val + jnp.where((lane & step) == 0, above, below)
    return x_val


def body(cfg, lat, w_in, b_in, b_conv, gain, shift, b_att, w_conv, w_att, out, hbuf, tbuf, u3, wbuf, wabuf, halo, stat_src, stat_rcv,
         ring, qbuf, acc, mx, ls, nbuf, kt, vbuf, obuf, par, bk_col, w_first, z_src, z_halo, z_col, z_tok,
         w_sem, wa_sem, st_send, st_recv, ha_send, ha_recv, rg_send, rg_recv, sw_send, sw_recv, o_send, o_recv, out_sem, z_send, z_recv):
    n_dev, n_rows, width, n_chan = cfg
    n_tok = n_rows * width
    lanes = n_chan // GROUPS
    n_vreg = n_chan // 128
    count = n_dev * n_tok * lanes
    me = lax.axis_index('cp')
    core = lax.rem(me, 2)
    mate = me + 1 - 2 * core
    ahead = lax.rem(me + 2, n_dev)
    behind = lax.rem(me + n_dev - 2, n_dev)
    below = lax.rem(me + 1, n_dev)
    above = lax.rem(me + n_dev - 1, n_dev)

    barrier = pltpu.get_barrier_semaphore()
    for dist in range(1, n_dev):
        pl.semaphore_signal(barrier, inc=1, device_id={'cp': lax.rem(me + dist, n_dev)}, device_id_type=MESH)

    def load_weights(idx):
        return pltpu.make_async_copy(w_conv.at[idx], wbuf.at[idx % 2], w_sem.at[idx % 2])

    load_weights(0).start()
    load_weights(1).start()
    load_att = pltpu.make_async_copy(w_att, wabuf, wa_sem)
    load_att.start()

    par[...] = jnp.zeros(par.shape, F32)
    par[B_IN:B_IN + 1, :] = b_in[...].astype(F32)
    par[B_CONV:B_CONV + 4, :] = b_conv[...].astype(F32)
    par[GAIN:GAIN + 5, :] = gain[...].astype(F32)
    par[SHIFT:SHIFT + 5, :] = shift[...].astype(F32)
    par[B_ATT:B_ATT + 4, :] = b_att[...].astype(F32)

    def row_of(idx):
        return par[pl.ds(idx, 1), :]

    def remote(src, dst, send_sem, recv_sem, dev):
        return pltpu.make_async_remote_copy(src_ref=src, dst_ref=dst, send_sem=send_sem, recv_sem=recv_sem,
                                            device_id={'cp': dev}, device_id_type=MESH)

    def partial(val):
        parts = val.reshape(val.shape[0] // 8, 8, n_chan)
        return jnp.sum(parts, axis=0), jnp.sum(parts * parts, axis=0)

    def send_stats(exch, smp, sums):
        row = lax.broadcasted_iota(jnp.int32, (8, n_chan), 0)
        first = jnp.sum(sums[0], axis=0, keepdims=True)
        second = jnp.sum(sums[1], axis=0, keepdims=True)
        both = jnp.where(row == 0, first, jnp.where(row == 1, second, 0.0))
        both = group_total(both, (1, 2, 4, 8))
        lane = lax.broadcasted_iota(jnp.int32, (8, 128), 1)
        packed = both[:, :128]
        for idx in range(1, n_vreg):
            packed = jnp.where((lane & 3) == idx, both[:, idx * 128:(idx + 1) * 128], packed)
        stat_src[exch, smp] = packed
        for dist in range(1, n_dev):
            remote(stat_src.at[exch, smp], stat_rcv.at[exch, smp, dist - 1], st_send.at[exch, smp],
                   st_recv.at[exch, smp], lax.rem(me + dist, n_dev)).start()

    def wait_stats(exch, smp):
        every = stat_rcv.at[exch, smp]
        pltpu.make_async_copy(every, every, st_recv.at[exch, smp]).wait()
        pltpu.make_async_copy(every, every, st_send.at[exch, smp]).wait()

    def affine(exch, smp, norm):
        total = stat_src[exch, smp] + jnp.sum(stat_rcv[exch, smp], axis=0)
        lane = lax.broadcasted_iota(jnp.int32, (8, 128), 1)
        spread = [group_total(jnp.where((lane & 3) == idx, total, 0.0), (1, 2)) for idx in range(n_vreg)]
        full = jnp.concatenate(spread, axis=1)
        mean = full[0:1, :] / count
        inv = lax.rsqrt(full[1:2, :] / count - mean * mean + GN_EPS)
        mul = inv * row_of(GAIN + norm)
        return mul, row_of(SHIFT + norm) - mean * mul

    def halo_copies(exch, smp, buf):
        top = remote(buf.at[smp, pl.ds(0, width)], halo.at[exch, smp, 1], ha_send.at[exch, smp, 0], ha_recv.at[exch, smp, 1], above)
        bottom = remote(buf.at[smp, pl.ds(n_tok - width, width)], halo.at[exch, smp, 0], ha_send.at[exch, smp, 1], ha_recv.at[exch, smp, 0], below)
        return top, bottom

    def send_halo(exch, smp, buf):
        for copy in halo_copies(exch, smp, buf):
            copy.start()

    def wait_halo(exch, smp, buf):
        for copy in halo_copies(exch, smp, buf):
            copy.wait()

    def conv_sample(smp, conv, norm, exch, hexch, src, dst, res):
        wait_stats(exch, smp)
        wait_halo(hexch, smp, src)
        mul, add = affine(exch, smp, norm)
        col = lax.broadcasted_iota(jnp.int32, (width, n_chan), 0)

        def put(row, x_val, keep):
            y_val = x_val.astype(F32) * mul + add
            half = 0.5 * y_val
            act = half + half * jnp.tanh(half)
            if keep is not None:
                act = jnp.where(keep, act, 0.0)
            left = jnp.where(col == 0, 0.0, pltpu.roll(act, 1, 0))
            right = jnp.where(col == width - 1, 0.0, pltpu.roll(act, width - 1, 0))
            u3[pl.ds(row * width, width), :n_chan] = left.astype(BF16)
            u3[pl.ds(row * width, width), n_chan:2 * n_chan] = act.astype(BF16)
            u3[pl.ds(row * width, width), 2 * n_chan:] = right.astype(BF16)

        def put_row(row, carry):
            put(row + 1, src[smp, pl.ds(row * width, width), :], None)
            return carry

        put(0, halo[hexch, smp, 0], me > 0)
        half_rows = n_rows // 2
        lax.fori_loop(0, half_rows + 1, put_row, 0)
        span = half_rows * width
        bias = row_of(B_CONV + conv)
        taps = 3 * n_chan
        sums = [jnp.zeros((8, n_chan), F32)] * 2
        for idx in range(2):
            base = idx * span
            total = bias
            for dy in range(3):
                start = base + dy * width
                total = total + jnp.dot(u3[start:start + span, :], wbuf[conv % 2, dy * taps:(dy + 1) * taps, :], preferred_element_type=F32)
            if idx == 0:
                for row in range(half_rows + 1, n_rows):
                    put_row(row, 0)
                put(n_rows + 1, halo[hexch, smp, 1], me < n_dev - 1)
            if res is not None:
                total = total + res[smp, base:base + span, :].astype(F32)
            rounded = total.astype(BF16)
            dst[smp, base:base + span, :] = rounded
            sums = [old + new for old, new in zip(sums, partial(rounded.astype(F32)))]
        return sums

    n_z = lat.shape[2]
    rows = [jnp.concatenate([lat[0, row].astype(F32), lat[1, row].astype(F32)], axis=0) for row in range(n_rows)]
    z_src[0] = rows[0]
    z_src[1] = rows[-1]
    blank = jnp.zeros((n_z, n_chan), F32)
    for smp in range(2):
        pieces = []
        for tap in range(9):
            pair = [blank, blank]
            pair[smp] = w_in[tap].astype(F32)
            pieces += pair
        pieces.append(jnp.zeros((128 - 18 * n_z, n_chan), F32))
        w_first[smp] = jnp.concatenate(pieces, axis=0).astype(BF16)
    pl.semaphore_wait(barrier, n_dev - 1)
    z_copies = (remote(z_src.at[0], z_halo.at[1], z_send.at[0], z_recv.at[1], above),
                remote(z_src.at[1], z_halo.at[0], z_send.at[1], z_recv.at[0], below))
    for copy in z_copies:
        copy.start()
    for copy in z_copies:
        copy.wait()
    rows = [jnp.where(me > 0, z_halo[0], 0.0)] + rows + [jnp.where(me < n_dev - 1, z_halo[1], 0.0)]
    lane = lax.broadcasted_iota(jnp.int32, (2 * n_z, width), 1)
    for tap in range(9):
        dy, dx = tap // 3, tap % 3
        moved = rows[dy:dy + n_rows]
        if dx == 0:
            moved = [jnp.where(lane == 0, 0.0, pltpu.roll(row, 1, 1)) for row in moved]
        if dx == 2:
            moved = [jnp.where(lane == width - 1, 0.0, pltpu.roll(row, width - 1, 1)) for row in moved]
        z_col[tap * 2 * n_z:(tap + 1) * 2 * n_z, :] = jnp.concatenate(moved, axis=1)
    z_col[18 * n_z:, :] = jnp.zeros((128 - 18 * n_z, n_tok), F32)
    z_tok[...] = jnp.transpose(z_col[...]).astype(BF16)

    def first(smp, carry):
        total = jnp.dot(z_tok[...], w_first[smp], preferred_element_type=F32) + row_of(B_IN)
        rounded = total.astype(BF16)
        hbuf[smp] = rounded
        send_halo(0, smp, hbuf)
        send_stats(0, smp, partial(rounded.astype(F32)))
        return carry

    lax.fori_loop(0, 2, first, 0)

    load_weights(0).wait()

    def stage0(smp, carry):
        sums = conv_sample(smp, 0, 0, 0, 0, hbuf, tbuf, None)
        send_halo(1, smp, tbuf)
        send_stats(1, smp, sums)
        return carry

    lax.fori_loop(0, 2, stage0, 0)
    load_weights(2).start()
    load_weights(1).wait()

    def forward(idx):
        return remote(ring.at[idx], ring.at[idx + 2], rg_send.at[0, idx], rg_recv.at[idx + 2], ahead)

    def backward(idx):
        src = 1 - idx if isinstance(idx, int) and idx < 2 else idx + 7
        return remote(ring.at[src], ring.at[idx + 9], rg_send.at[1, idx], rg_recv.at[idx + 9], behind)

    def swap():
        return remote(hbuf.at[1 - core], ring.at[1], sw_send, sw_recv, mate)

    def stage1(smp, carry):
        sums = conv_sample(smp, 1, 1, 1, 1, tbuf, hbuf, hbuf)
        send_stats(2, smp, sums)

        @pl.when(smp == 1 - core)
        def _():
            swap().start()

        @pl.when(smp == core)
        def _():
            ring[0] = hbuf[smp]
            forward(0).start()
            backward(1).start()

        return carry

    lax.fori_loop(0, 2, stage1, 0)
    load_weights(3).start()
    swap().wait()
    forward(1).start()
    backward(0).start()
    load_att.wait()
    wabuf[1] = jnp.transpose(wabuf[1].astype(F32)).astype(BF16)
    bk_col[...] = jnp.transpose(jnp.broadcast_to(row_of(B_ATT + 1), (128, n_chan)))

    wait_stats(2, core)
    wait_stats(2, 1 - core)
    mul2, add2 = affine(2, core, 2)
    scale = n_chan ** -0.5 * math.log2(math.e)
    mx[...] = jnp.full(mx.shape, -jnp.inf, F32)
    ls[...] = jnp.zeros(ls.shape, F32)
    acc[...] = jnp.zeros(acc.shape, F32)

    def norm_slot(slot):
        nbuf[...] = (ring[slot].astype(F32) * mul2 + add2).astype(BF16)

    def query(slot, carry):
        norm_slot(slot)
        proj = jnp.dot(nbuf[...], wabuf[0], preferred_element_type=F32) + row_of(B_ATT)
        qbuf[pl.ds(slot * n_tok, n_tok), :] = proj.astype(BF16)
        return carry

    lax.fori_loop(0, 2, query, 0)
    q_len = n_tok // 2

    def attend(slot):
        norm_slot(slot)
        keys = lax.dot_general(wabuf[1], nbuf[...], (((1,), (1,)), ((), ())), preferred_element_type=F32)
        kt[...] = (keys + bk_col[:, 0:1]).astype(BF16)
        vals = jnp.dot(nbuf[...], wabuf[2], preferred_element_type=F32) + row_of(B_ATT + 2)
        vbuf[...] = vals.astype(BF16)

        def score(blk):
            return jnp.dot(qbuf[blk * q_len:(blk + 1) * q_len, :], kt[...], preferred_element_type=F32)

        n_part = max(n_tok // 128, 1)
        wide = n_tok // n_part
        scores = score(0)
        for blk in range(4):
            following = score(blk + 1) if blk < 3 else None
            rows = slice(blk * q_len, (blk + 1) * q_len)
            cols = [scores[:, idx * wide:(idx + 1) * wide] for idx in range(n_part)]
            old = mx[rows, :]
            new = jnp.maximum(old, jnp.max(functools.reduce(jnp.maximum, cols), axis=1, keepdims=True) * scale)
            fade = jnp.exp2(old - new)
            prob = [jnp.exp2(col * scale - new[:, :wide]) for col in cols]
            mx[rows, :] = new
            ls[rows, :wide] = ls[rows, :wide] * fade[:, :wide] + functools.reduce(jnp.add, prob)
            prob = jnp.concatenate([col.astype(BF16) for col in prob], axis=1)
            acc[rows, :] = acc[rows, :] * fade[:, 0:1] + jnp.dot(prob, vbuf[...], preferred_element_type=F32)
            scores = following

    def own(slot, carry):
        attend(slot)
        return carry

    lax.fori_loop(0, 2, own, 0)

    def step(idx, carry):
        forward(idx - 1).wait_recv()

        @pl.when(idx <= 5)
        def _():
            forward(idx + 1).start()

        remote(ring.at[idx + 8], ring.at[idx + 8], rg_send.at[1, idx - 1], rg_recv.at[idx + 8], behind).wait_recv()

        @pl.when(idx <= 5)
        def _():
            backward(idx + 1).start()

        def both(side, inner):
            attend(idx + 1 + 7 * side)
            return inner

        return lax.fori_loop(0, 2, both, carry)

    lax.fori_loop(1, 8, step, 0)

    def drain(idx, carry):
        forward(idx).wait_send()
        remote(ring.at[0], ring.at[9], rg_send.at[1, idx], rg_recv.at[9], behind).wait_send()
        return carry

    lax.fori_loop(0, 7, drain, 0)

    def finish(base):
        total = jnp.sum(ls[base:base + n_tok, :], axis=1, keepdims=True)
        return (acc[base:base + n_tok, :] / total).astype(BF16)

    vbuf[...] = finish(n_tok)
    give = remote(vbuf, obuf.at[1], o_send, o_recv, mate)
    give.start()
    obuf[0] = finish(0)

    def project(side, carry):
        @pl.when(side == 1)
        def _():
            give.wait()

        smp = lax.rem(core + side, 2)
        total = jnp.dot(obuf[side], wabuf[3], preferred_element_type=F32) + row_of(B_ATT + 3)
        rounded = (hbuf[smp].astype(F32) + total).astype(BF16)
        hbuf[smp] = rounded
        send_halo(2, smp, hbuf)
        send_stats(3, smp, partial(rounded.astype(F32)))
        return carry

    lax.fori_loop(0, 2, project, 0)
    load_weights(2).wait()

    def stage2(smp, carry):
        sums = conv_sample(smp, 2, 3, 3, 2, hbuf, tbuf, None)
        send_halo(3, smp, tbuf)
        send_stats(4, smp, sums)
        return carry

    lax.fori_loop(0, 2, stage2, 0)
    load_weights(3).wait()

    def write(smp):
        return pltpu.make_async_copy(tbuf.at[smp], out.at[smp], out_sem.at[smp])

    def stage3(smp, carry):
        conv_sample(smp, 3, 4, 4, 3, tbuf, tbuf, hbuf)
        write(smp).start()
        return carry

    lax.fori_loop(0, 2, stage3, 0)
    write(0).wait()
    write(1).wait()


def decoder(n_dev, lat, w_in, b_in, b_conv, gain, shift, b_att, w_conv, w_att):
    n_rows, n_z, width = lat.shape[1:]
    n_chan = w_in.shape[-1]
    n_tok = n_rows * width
    vmem = pltpu.VMEM
    dma = pltpu.SemaphoreType.DMA
    in_vmem = pl.BlockSpec(memory_space=pltpu.VMEM)
    in_any = pl.BlockSpec(memory_space=pl.ANY)
    scratch = [
        vmem((2, n_tok, n_chan), BF16),
        vmem((2, n_tok, n_chan), BF16),
        vmem((n_tok + 2 * width, 3 * n_chan), BF16),
        vmem((2, 9 * n_chan, n_chan), BF16),
        vmem((4, n_chan, n_chan), BF16),
        vmem((4, 2, 2, width, n_chan), BF16),
        vmem((5, 2, 8, 128), F32),
        vmem((5, 2, n_dev - 1, 8, 128), F32),
        vmem((n_dev, n_tok, n_chan), BF16),
        vmem((2 * n_tok, n_chan), BF16),
        vmem((2 * n_tok, n_chan), F32),
        vmem((2 * n_tok, 128), F32),
        vmem((2 * n_tok, 128), F32),
        vmem((n_tok, n_chan), BF16),
        vmem((n_chan, n_tok), BF16),
        vmem((n_tok, n_chan), BF16),
        vmem((2, n_tok, n_chan), BF16),
        vmem((N_PAR, n_chan), F32),
        vmem((n_chan, 128), F32),
        vmem((2, 128, n_chan), BF16),
        vmem((2, 2 * n_z, width), F32),
        vmem((2, 2 * n_z, width), F32),
        vmem((128, n_tok), F32),
        vmem((n_tok, 128), BF16),
        dma((2,)), dma, dma((5, 2)), dma((5, 2)), dma((4, 2, 2)), dma((4, 2, 2)), dma((2, 7)), dma((16,)),
        dma, dma, dma, dma, dma((2,)), dma((2,)), dma((2,)),
    ]
    return pl.pallas_call(
        functools.partial(body, (n_dev, n_rows, width, n_chan)),
        out_shape=jax.ShapeDtypeStruct((2, n_tok, n_chan), BF16),
        in_specs=[in_vmem] * 7 + [in_any] * 2,
        out_specs=in_any,
        scratch_shapes=scratch,
        compiler_params=pltpu.CompilerParams(collective_id=0, has_side_effects=True, vmem_limit_bytes=67043328),
    )(lat, w_in, b_in, b_conv, gain, shift, b_att, w_conv, w_att)


def solution(mesh):
    n_dev = mesh.shape['cp']

    def local_fn(latents, w_in, b_in, w_conv, b_conv, gn_scale, gn_shift, w_attn, b_attn):
        n_batch, n_rows, width, n_z = latents.shape
        n_chan = w_in.shape[-1]
        out = decoder(n_dev, latents.transpose(0, 1, 3, 2), w_in.reshape(9, n_z, n_chan), b_in.reshape(1, n_chan), b_conv, gn_scale,
                      gn_shift, b_attn, w_conv.reshape(4, 9 * n_chan, n_chan), w_attn)
        return out.reshape(n_batch, n_rows, width, n_chan)

    band_spec = P('dp', 'cp')
    whole_spec = P()
    return jax.shard_map(local_fn, mesh=mesh, in_specs=(band_spec,) + (whole_spec,) * 8, out_specs=band_spec, check_vma=False)
```

```python
import functools
import math

import jax
import jax.numpy as jnp
from jax import lax
from jax.experimental import pallas as pl
from jax.experimental.pallas import tpu as pltpu
from jax.sharding import PartitionSpec as P

F32 = jnp.float32
BF16 = jnp.bfloat16
GROUPS = 32
GN_EPS = 1e-6
MESH = pl.DeviceIdType.MESH
B_IN, B_CONV, GAIN, SHIFT, B_ATT, N_PAR = 0, 1, 5, 10, 15, 24


def group_total(x_val, steps):
    lane = lax.broadcasted_iota(jnp.int32, x_val.shape, 1)
    width = x_val.shape[1]
    for step in steps:
        above = pltpu.roll(x_val, width - step, 1)
        below = pltpu.roll(x_val, step, 1)
        x_val = x_val + jnp.where((lane & step) == 0, above, below)
    return x_val


def body(cfg, lat, w_in, b_in, b_conv, gain, shift, b_att, w_conv, w_att, out, hbuf, tbuf, u3, wbuf, wabuf, halo, stat_src, stat_rcv,
         ring, qbuf, acc, mx, ls, nbuf, kt, vbuf, obuf, par, bk_col, w_first, z_src, z_halo, z_col, z_tok, z_far, far_in, far_mid,
         w_sem, wa_sem, st_send, st_recv, ha_send, ha_recv, rg_send, rg_recv, sw_send, sw_recv, o_send, o_recv, out_sem, z_send, z_recv, zf_send, zf_recv):
    n_dev, n_rows, width, n_chan = cfg
    n_tok = n_rows * width
    lanes = n_chan // GROUPS
    n_vreg = n_chan // 128
    count = n_dev * n_tok * lanes
    me = lax.axis_index('cp')
    core = lax.rem(me, 2)
    mate = me + 1 - 2 * core
    ahead = lax.rem(me + 2, n_dev)
    behind = lax.rem(me + n_dev - 2, n_dev)
    below = lax.rem(me + 1, n_dev)
    above = lax.rem(me + n_dev - 1, n_dev)

    barrier = pltpu.get_barrier_semaphore()
    for dist in range(1, n_dev):
        pl.semaphore_signal(barrier, inc=1, device_id={'cp': lax.rem(me + dist, n_dev)}, device_id_type=MESH)

    def load_weights(idx):
        return pltpu.make_async_copy(w_conv.at[idx], wbuf.at[idx % 2], w_sem.at[idx % 2])

    load_weights(0).start()
    load_weights(1).start()
    load_att = pltpu.make_async_copy(w_att, wabuf, wa_sem)
    load_att.start()

    par[...] = jnp.zeros(par.shape, F32)
    par[B_IN:B_IN + 1, :] = b_in[...].astype(F32).reshape(1, n_chan)
    par[B_CONV:B_CONV + 4, :] = b_conv[...].astype(F32)
    par[GAIN:GAIN + 5, :] = gain[...].astype(F32)
    par[SHIFT:SHIFT + 5, :] = shift[...].astype(F32)
    par[B_ATT:B_ATT + 4, :] = b_att[...].astype(F32)

    def row_of(idx):
        return par[pl.ds(idx, 1), :]

    def remote(src, dst, send_sem, recv_sem, dev):
        return pltpu.make_async_remote_copy(src_ref=src, dst_ref=dst, send_sem=send_sem, recv_sem=recv_sem,
                                            device_id={'cp': dev}, device_id_type=MESH)

    def partial(val):
        parts = val.reshape(val.shape[0] // 8, 8, n_chan)
        return jnp.sum(parts, axis=0), jnp.sum(parts * parts, axis=0)

    def send_stats(exch, smp, sums):
        row = lax.broadcasted_iota(jnp.int32, (8, n_chan), 0)
        first = jnp.sum(sums[0], axis=0, keepdims=True)
        second = jnp.sum(sums[1], axis=0, keepdims=True)
        both = jnp.where(row == 0, first, jnp.where(row == 1, second, 0.0))
        both = group_total(both, (1, 2, 4, 8))
        lane = lax.broadcasted_iota(jnp.int32, (8, 128), 1)
        packed = both[:, :128]
        for idx in range(1, n_vreg):
            packed = jnp.where((lane & 3) == idx, both[:, idx * 128:(idx + 1) * 128], packed)
        stat_src[exch, smp] = packed
        for dist in range(1, n_dev):
            remote(stat_src.at[exch, smp], stat_rcv.at[exch, smp, dist - 1], st_send.at[exch, smp],
                   st_recv.at[exch, smp], lax.rem(me + dist, n_dev)).start()

    def wait_stats(exch, smp):
        every = stat_rcv.at[exch, smp]
        pltpu.make_async_copy(every, every, st_recv.at[exch, smp]).wait()
        pltpu.make_async_copy(every, every, st_send.at[exch, smp]).wait()

    def affine(exch, smp, norm):
        total = stat_src[exch, smp] + jnp.sum(stat_rcv[exch, smp], axis=0)
        lane = lax.broadcasted_iota(jnp.int32, (8, 128), 1)
        spread = [group_total(jnp.where((lane & 3) == idx, total, 0.0), (1, 2)) for idx in range(n_vreg)]
        full = jnp.concatenate(spread, axis=1)
        mean = full[0:1, :] / count
        inv = lax.rsqrt(full[1:2, :] / count - mean * mean + GN_EPS)
        mul = inv * row_of(GAIN + norm)
        return mul, row_of(SHIFT + norm) - mean * mul

    def halo_copies(exch, smp, buf):
        top = remote(buf.at[smp, pl.ds(0, width)], halo.at[exch, smp, 1], ha_send.at[exch, smp, 0], ha_recv.at[exch, smp, 1], above)
        bottom = remote(buf.at[smp, pl.ds(n_tok - width, width)], halo.at[exch, smp, 0], ha_send.at[exch, smp, 1], ha_recv.at[exch, smp, 0], below)
        return top, bottom

    def send_halo(exch, smp, buf):
        for copy in halo_copies(exch, smp, buf):
            copy.start()

    def wait_halo(exch, smp, buf):
        for copy in halo_copies(exch, smp, buf):
            copy.wait()

    col = lax.broadcasted_iota(jnp.int32, (width, n_chan), 0)
    taps = 3 * n_chan

    def conv_core(rows_out, edge, load, keep_top, keep_bottom, mul, add, conv, res, store):
        def put(row, keep):
            half = 0.5 * (load(row).astype(F32) * mul + add)
            act = half + half * jnp.tanh(half)
            if keep is not None:
                act = jnp.where(keep, act, 0.0)
            left = jnp.where(col == 0, 0.0, pltpu.roll(act, 1, 0))
            right = jnp.where(col == width - 1, 0.0, pltpu.roll(act, width - 1, 0))
            u3[pl.ds(row * width, width), :n_chan] = left.astype(BF16)
            u3[pl.ds(row * width, width), n_chan:2 * n_chan] = act.astype(BF16)
            u3[pl.ds(row * width, width), 2 * n_chan:] = right.astype(BF16)

        def put_row(row, carry):
            put(row, None)
            return carry

        half_rows = rows_out // 2

        def put_top(row, carry):
            put(row, keep_top)
            return carry

        if edge == 1:
            put(0, keep_top)
        else:
            lax.fori_loop(0, edge, put_top, 0)
        lax.fori_loop(edge, half_rows + 2, put_row, 0)
        span = half_rows * width
        bias = row_of(B_CONV + conv)
        sums = [jnp.zeros((8, n_chan), F32)] * 2
        for idx in range(2):
            base = idx * span
            total = bias
            for dy in range(3):
                start = base + dy * width
                total = total + jnp.dot(u3[start:start + span, :], wbuf[conv % 2, dy * taps:(dy + 1) * taps, :], preferred_element_type=F32)
            if idx == 0:
                for row in range(half_rows + 2, rows_out + 2 - edge):
                    put(row, None)
                for row in range(rows_out + 2 - edge, rows_out + 2):
                    put(row, keep_bottom)
            if res is not None:
                total = total + res(base, span).astype(F32)
            rounded = total.astype(BF16)
            store(base, span, rounded)
            sums = [old + new for old, new in zip(sums, partial(rounded.astype(F32)))]
        return sums

    def conv_sample(smp, conv, norm, exch, hexch, src, dst, res):
        wait_stats(exch, smp)
        wait_halo(hexch, smp, src)
        mul, add = affine(exch, smp, norm)

        def load(row):
            if isinstance(row, int) and row == 0:
                return halo[hexch, smp, 0]
            if isinstance(row, int) and row == n_rows + 1:
                return halo[hexch, smp, 1]
            return src[smp, pl.ds((row - 1) * width, width), :]

        def store(base, span, val):
            dst[smp, base:base + span, :] = val

        get = None if res is None else lambda base, span: res[smp, base:base + span, :]
        return conv_core(n_rows, 1, load, me > 0, me < n_dev - 1, mul, add, conv, get, store)

    n_z = lat.shape[2]
    rows = [jnp.concatenate([lat[0, row].astype(F32), lat[1, row].astype(F32)], axis=0) for row in range(n_rows)]
    z_src[0] = rows[0]
    z_src[1] = rows[-1]
    blank = jnp.zeros((n_z, n_chan), F32)
    for smp in range(2):
        pieces = []
        for tap in range(9):
            pair = [blank, blank]
            pair[smp] = w_in[tap].astype(F32)
            pieces += pair
        pieces.append(jnp.zeros((128 - 18 * n_z, n_chan), F32))
        w_first[smp] = jnp.concatenate(pieces, axis=0).astype(BF16)
    pl.semaphore_wait(barrier, n_dev - 1)
    z_copies = (remote(z_src.at[0], z_halo.at[1], z_send.at[0], z_recv.at[1], above),
                remote(z_src.at[1], z_halo.at[0], z_send.at[1], z_recv.at[0], below))
    for copy in z_copies:
        copy.start()
    half_ring = n_dev // 2
    base_dev = me - core + half_ring
    side_dev = base_dev + 4 * core - 2
    far_copies = []
    for smp in range(2):
        far_copies.append(remote(lat.at[smp], z_far.at[1 + core], zf_send.at[smp], zf_recv.at[1 + core], lax.rem(base_dev + smp, n_dev)))
        far_copies.append(remote(lat.at[smp], z_far.at[3 - 3 * core], zf_send.at[2 + smp], zf_recv.at[3 - 3 * core],
                                 lax.rem(side_dev + smp, n_dev)))
    for copy in far_copies:
        copy.start()
    for copy in z_copies:
        copy.wait()
    rows = [jnp.where(me > 0, z_halo[0], 0.0)] + rows + [jnp.where(me < n_dev - 1, z_halo[1], 0.0)]
    lane = lax.broadcasted_iota(jnp.int32, (2 * n_z, width), 1)

    def columns(lines):
        n_out = len(lines) - 2
        for tap in range(9):
            dy, dx = tap // 3, tap % 3
            moved = lines[dy:dy + n_out]
            if dx == 0:
                moved = [jnp.where(lane == 0, 0.0, pltpu.roll(line, 1, 1)) for line in moved]
            if dx == 2:
                moved = [jnp.where(lane == width - 1, 0.0, pltpu.roll(line, width - 1, 1)) for line in moved]
            z_col[tap * 2 * n_z:(tap + 1) * 2 * n_z, :n_out * width] = jnp.concatenate(moved, axis=1)
        z_tok[:n_out * width, :] = jnp.transpose(z_col[:, :n_out * width]).astype(BF16)

    z_col[18 * n_z:, :] = jnp.zeros((128 - 18 * n_z, n_tok), F32)
    columns(rows)

    def first(smp, carry):
        total = jnp.dot(z_tok[...], w_first[smp], preferred_element_type=F32) + row_of(B_IN)
        rounded = total.astype(BF16)
        hbuf[smp] = rounded
        send_halo(0, smp, hbuf)
        send_stats(0, smp, partial(rounded.astype(F32)))
        return carry

    lax.fori_loop(0, 2, first, 0)

    load_weights(0).wait()

    def stage0(smp, carry):
        sums = conv_sample(smp, 0, 0, 0, 0, hbuf, tbuf, None)
        send_halo(1, smp, tbuf)
        send_stats(1, smp, sums)
        return carry

    lax.fori_loop(0, 2, stage0, 0)
    load_weights(1).wait()

    def forward(src, idx):
        slot = idx + 1 + idx // 5
        return remote(ring.at[src], ring.at[slot], rg_send.at[0, idx], rg_recv.at[slot], ahead)

    def backward(src, idx):
        return remote(ring.at[src], ring.at[idx + 9], rg_send.at[1, idx], rg_recv.at[idx + 9], behind)

    def arrived(slot):
        remote(ring.at[slot], ring.at[slot], rg_send.at[0, 0], rg_recv.at[slot], behind).wait_recv()

    def swap():
        return remote(hbuf.at[1 - core], ring.at[8], sw_send, sw_recv, mate)

    def stage1(smp, carry):
        sums = conv_sample(smp, 1, 1, 1, 1, tbuf, hbuf, hbuf)
        send_stats(2, smp, sums)

        @pl.when(smp == 1 - core)
        def _():
            swap().start()

        @pl.when(smp == core)
        def _():
            ring[0] = hbuf[smp]
            forward(0, 0).start()
            backward(0, 1).start()

        return carry

    lax.fori_loop(0, 2, stage1, 0)
    swap().wait()
    forward(8, 1).start()
    backward(8, 0).start()
    load_att.wait()
    wabuf[1] = jnp.transpose(wabuf[1].astype(F32)).astype(BF16)
    bk_col[...] = jnp.transpose(jnp.broadcast_to(row_of(B_ATT + 1), (128, n_chan)))

    wait_stats(2, core)
    wait_stats(2, 1 - core)
    mul2, add2 = affine(2, core, 2)
    scale = n_chan ** -0.5 * math.log2(math.e)
    q_len = n_tok // 2

    def clear(blk, carry):
        rows = pl.ds(blk * q_len, q_len)
        mx[rows, :] = jnp.full((q_len, 128), -jnp.inf, F32)
        ls[rows, :] = jnp.zeros((q_len, 128), F32)
        acc[rows, :] = jnp.zeros((q_len, n_chan), F32)
        return carry

    lax.fori_loop(0, 4, clear, 0)

    def norm_slot(slot):
        nbuf[...] = (ring[slot].astype(F32) * mul2 + add2).astype(BF16)

    def query(slot, carry):
        norm_slot(8 * slot)
        proj = jnp.dot(nbuf[...], wabuf[0], preferred_element_type=F32) + row_of(B_ATT)
        qbuf[pl.ds(slot * n_tok, n_tok), :] = proj.astype(BF16)
        return carry

    lax.fori_loop(0, 2, query, 0)

    def attend(slot):
        norm_slot(slot)
        keys = lax.dot_general(wabuf[1], nbuf[...], (((1,), (1,)), ((), ())), preferred_element_type=F32)
        kt[...] = (keys + bk_col[:, 0:1]).astype(BF16)
        vals = jnp.dot(nbuf[...], wabuf[2], preferred_element_type=F32) + row_of(B_ATT + 2)
        vbuf[...] = vals.astype(BF16)

        def score(blk):
            return jnp.dot(qbuf[blk * q_len:(blk + 1) * q_len, :], kt[...], preferred_element_type=F32)

        n_part = max(n_tok // 128, 1)
        wide = n_tok // n_part
        scores = score(0)
        for blk in range(4):
            following = score(blk + 1) if blk < 3 else None
            rows = slice(blk * q_len, (blk + 1) * q_len)
            cols = [scores[:, idx * wide:(idx + 1) * wide] for idx in range(n_part)]
            old = mx[rows, :]
            new = jnp.maximum(old, jnp.max(functools.reduce(jnp.maximum, cols), axis=1, keepdims=True) * scale)
            fade = jnp.exp2(old - new)
            prob = [jnp.exp2(col * scale - new[:, :wide]) for col in cols]
            mx[rows, :] = new
            ls[rows, :wide] = ls[rows, :wide] * fade[:, :wide] + functools.reduce(jnp.add, prob)
            prob = jnp.concatenate([col.astype(BF16) for col in prob], axis=1)
            acc[rows, :] = acc[rows, :] * fade[:, 0:1] + jnp.dot(prob, vbuf[...], preferred_element_type=F32)
            scores = following

    far = lax.rem(me - core + half_ring, n_dev)
    far_rows = n_rows + 4

    def far_first(part):
        band = far + part
        inside = (band > 0, band < n_dev - 1)

        @pl.when(part == 0)
        def _():
            for slot in range(4):
                remote(lat.at[0], z_far.at[slot], zf_send.at[slot], zf_recv.at[slot], mate).wait()

        blank_z = jnp.zeros((n_z, width), F32)

        def line(slot, row, keep):
            val = z_far[slot, row].astype(F32)
            if keep is not None:
                val = jnp.where(keep, val, 0.0)
            return jnp.concatenate([val, blank_z], axis=0)

        lines = [line(part, n_rows - 3 + row, inside[0]) for row in range(3)]
        lines += [line(part + 1, row, None) for row in range(n_rows)]
        lines += [line(part + 2, row, inside[1]) for row in range(3)]
        half_far = far_rows // 2
        for idx in range(2):
            columns(lines[idx * half_far:(idx + 1) * half_far + 2])
            total = jnp.dot(z_tok[:half_far * width, :], w_first[0], preferred_element_type=F32) + row_of(B_IN)
            far_in[idx * half_far * width:(idx + 1) * half_far * width, :] = total.astype(BF16)
        mul, add = affine(0, core, 0)

        def store(base, span, val):
            far_mid[base:base + span, :] = val

        conv_core(n_rows + 2, 2, lambda row: far_in[pl.ds(row * width, width), :], inside[0], inside[1], mul, add, 0, None, store)

    def far_second(part):
        band = far + part
        mul, add = affine(1, core, 1)

        def store(base, span, val):
            ring[6 + 9 * part, base:base + span, :] = val

        conv_core(n_rows, 1, lambda row: far_mid[pl.ds(row * width, width), :], band > 0, band < n_dev - 1, mul, add, 1,
                  lambda base, span: far_in[base + 2 * width:base + 2 * width + span, :], store)

    def step(idx, carry):
        half = idx // 2
        odd = idx % 2

        @pl.when((idx == 2) | (idx == 6))
        def _():
            far_first(idx // 4)

        @pl.when((idx == 4) | (idx == 8))
        def _():
            far_second(idx // 4 - 1)

        @pl.when(idx == 8)
        def _():
            load_weights(2).start()
            load_weights(3).start()

        @pl.when((odd == 0) & (idx >= 2) & (idx != 12))
        def _():
            arrived(half)

            @pl.when(idx <= 8)
            def _():
                forward(half, half + 1).start()

        @pl.when((odd == 1) & (idx >= 3) & (idx <= 13))
        def _():
            arrived(8 + half)

            @pl.when(idx <= 9)
            def _():
                backward(8 + half, half + 1).start()

        attend(half + 8 * odd)
        return carry

    lax.fori_loop(0, n_dev, step, 0)

    def drain(idx, carry):
        forward(0, idx).wait_send()
        backward(0, idx).wait_send()
        return carry

    lax.fori_loop(0, 6, drain, 0)

    def finish(base, put_out):
        part = q_len // 2

        def one(blk, carry):
            rows = pl.ds(base + blk * part, part)
            total = jnp.sum(ls[rows, :], axis=1, keepdims=True)
            put_out(pl.ds(blk * part, part), (acc[rows, :] / total).astype(BF16))
            return carry

        lax.fori_loop(0, 4, one, 0)

    def to_mate(rows, val):
        vbuf[rows, :] = val

    def to_self(rows, val):
        obuf[0, rows, :] = val

    finish(n_tok, to_mate)
    give = remote(vbuf, obuf.at[1], o_send, o_recv, mate)
    give.start()
    finish(0, to_self)

    def project(side, carry):
        @pl.when(side == 1)
        def _():
            give.wait()

        smp = lax.rem(core + side, 2)
        total = jnp.dot(obuf[side], wabuf[3], preferred_element_type=F32) + row_of(B_ATT + 3)
        rounded = (hbuf[smp].astype(F32) + total).astype(BF16)
        hbuf[smp] = rounded
        send_halo(2, smp, hbuf)
        send_stats(3, smp, partial(rounded.astype(F32)))
        return carry

    lax.fori_loop(0, 2, project, 0)
    load_weights(2).wait()

    def stage2(smp, carry):
        sums = conv_sample(smp, 2, 3, 3, 2, hbuf, tbuf, None)
        send_halo(3, smp, tbuf)
        send_stats(4, smp, sums)
        return carry

    lax.fori_loop(0, 2, stage2, 0)
    load_weights(3).wait()

    def write(smp):
        return pltpu.make_async_copy(tbuf.at[smp], out.at[smp], out_sem.at[smp])

    def stage3(smp, carry):
        conv_sample(smp, 3, 4, 4, 3, tbuf, tbuf, hbuf)
        write(smp).start()
        return carry

    lax.fori_loop(0, 2, stage3, 0)
    write(0).wait()
    write(1).wait()


def decoder(n_dev, lat, w_in, b_in, b_conv, gain, shift, b_att, w_conv, w_att):
    n_rows, n_z, width = lat.shape[1:]
    n_chan = w_in.shape[-1]
    n_tok = n_rows * width
    vmem = pltpu.VMEM
    dma = pltpu.SemaphoreType.DMA
    in_vmem = pl.BlockSpec(memory_space=pltpu.VMEM)
    in_any = pl.BlockSpec(memory_space=pl.ANY)
    scratch = [
        vmem((2, n_tok, n_chan), BF16),
        vmem((2, n_tok, n_chan), BF16),
        vmem((n_tok + 4 * width, 3 * n_chan), BF16),
        vmem((2, 9 * n_chan, n_chan), BF16),
        vmem((4, n_chan, n_chan), BF16),
        vmem((4, 2, 2, width, n_chan), BF16),
        vmem((5, 2, 8, 128), F32),
        vmem((5, 2, n_dev - 1, 8, 128), F32),
        vmem((n_dev, n_tok, n_chan), BF16),
        vmem((2 * n_tok, n_chan), BF16),
        vmem((2 * n_tok, n_chan), F32),
        vmem((2 * n_tok, 128), F32),
        vmem((2 * n_tok, 128), F32),
        vmem((n_tok, n_chan), BF16),
        vmem((n_chan, n_tok), BF16),
        vmem((n_tok, n_chan), BF16),
        vmem((2, n_tok, n_chan), BF16),
        vmem((N_PAR, n_chan), F32),
        vmem((n_chan, 128), F32),
        vmem((2, 128, n_chan), BF16),
        vmem((2, 2 * n_z, width), F32),
        vmem((2, 2 * n_z, width), F32),
        vmem((128, n_tok), F32),
        vmem((n_tok, 128), BF16),
        vmem((4, n_rows, n_z, width), BF16),
        vmem((n_tok + 4 * width, n_chan), BF16),
        vmem((n_tok + 2 * width, n_chan), BF16),
        dma((2,)), dma, dma((5, 2)), dma((5, 2)), dma((4, 2, 2)), dma((4, 2, 2)), dma((2, 6)), dma((n_dev,)),
        dma, dma, dma, dma, dma((2,)), dma((2,)), dma((2,)), dma((4,)), dma((4,)),
    ]
    return pl.pallas_call(
        functools.partial(body, (n_dev, n_rows, width, n_chan)),
        out_shape=jax.ShapeDtypeStruct((2, n_tok, n_chan), BF16),
        in_specs=[in_vmem] * 7 + [in_any] * 2,
        out_specs=in_any,
        scratch_shapes=scratch,
        compiler_params=pltpu.CompilerParams(collective_id=0, has_side_effects=True, vmem_limit_bytes=67043328),
    )(lat, w_in, b_in, b_conv, gain, shift, b_att, w_conv, w_att)


def solution(mesh):
    n_dev = mesh.shape['cp']

    def local_fn(latents, w_in, b_in, w_conv, b_conv, gn_scale, gn_shift, w_attn, b_attn):
        n_batch, n_rows, width, n_z = latents.shape
        n_chan = w_in.shape[-1]
        out = decoder(n_dev, latents.transpose(0, 1, 3, 2), w_in.reshape(9, n_z, n_chan), b_in, b_conv, gn_scale,
                      gn_shift, b_attn, w_conv.reshape(4, 9 * n_chan, n_chan), w_attn)
        return out.reshape(n_batch, n_rows, width, n_chan)

    band_spec = P('dp', 'cp')
    whole_spec = P()
    return jax.shard_map(local_fn, mesh=mesh, in_specs=(band_spec,) + (whole_spec,) * 8, out_specs=band_spec, check_vma=False)
```

```python
import functools
import math

import jax
import jax.numpy as jnp
from jax import lax
from jax.experimental import pallas as pl
from jax.experimental.pallas import tpu as pltpu
from jax.sharding import PartitionSpec as P

F32 = jnp.float32
BF16 = jnp.bfloat16
GROUPS = 32
GN_EPS = 1e-6
MESH = pl.DeviceIdType.MESH
B_IN, B_CONV, GAIN, SHIFT, B_ATT, NORM_ATT, N_PAR = 0, 1, 5, 10, 15, 19, 24


def group_total(x_val, steps):
    lane = lax.broadcasted_iota(jnp.int32, x_val.shape, 1)
    width = x_val.shape[1]
    for step in steps:
        above = pltpu.roll(x_val, width - step, 1)
        below = pltpu.roll(x_val, step, 1)
        x_val = x_val + jnp.where((lane & step) == 0, above, below)
    return x_val


def body(cfg, lat, w_in, b_in, b_conv, gain, shift, b_att, w_conv, w_att, out, hbuf, tbuf, u3, wbuf, wabuf, halo, stat_src, stat_rcv,
         ring, qbuf, acc, mx, ls, nbuf, kt, vbuf, obuf, par, bk_col, w_first, z_src, z_halo, z_col, z_tok, z_far, far_in, far_mid,
         w_sem, wa_sem, st_send, st_recv, ha_send, ha_recv, rg_send, rg_recv, sw_send, sw_recv, o_send, o_recv, out_sem, z_send, z_recv, zf_send, zf_recv):
    n_dev, n_rows, width, n_chan = cfg
    n_tok = n_rows * width
    lanes = n_chan // GROUPS
    n_vreg = n_chan // 128
    count = n_dev * n_tok * lanes
    me = lax.axis_index('cp')
    core = lax.rem(me, 2)
    mate = me + 1 - 2 * core
    ahead = lax.rem(me + 2, n_dev)
    behind = lax.rem(me + n_dev - 2, n_dev)
    below = lax.rem(me + 1, n_dev)
    above = lax.rem(me + n_dev - 1, n_dev)

    barrier = pltpu.get_barrier_semaphore()
    for dist in range(1, n_dev):
        pl.semaphore_signal(barrier, inc=1, device_id={'cp': lax.rem(me + dist, n_dev)}, device_id_type=MESH)

    def load_weights(idx):
        return pltpu.make_async_copy(w_conv.at[idx], wbuf.at[idx % 2], w_sem.at[idx % 2])

    load_weights(0).start()
    load_weights(1).start()
    load_att = pltpu.make_async_copy(w_att, wabuf, wa_sem)
    load_att.start()

    par[...] = jnp.zeros(par.shape, F32)
    par[B_IN:B_IN + 1, :] = b_in[...].astype(F32).reshape(1, n_chan)
    par[B_CONV:B_CONV + 4, :] = b_conv[...].astype(F32)
    par[GAIN:GAIN + 5, :] = gain[...].astype(F32)
    par[SHIFT:SHIFT + 5, :] = shift[...].astype(F32)
    par[B_ATT:B_ATT + 4, :] = b_att[...].astype(F32)

    def row_of(idx):
        return par[pl.ds(idx, 1), :]

    def remote(src, dst, send_sem, recv_sem, dev):
        return pltpu.make_async_remote_copy(src_ref=src, dst_ref=dst, send_sem=send_sem, recv_sem=recv_sem,
                                            device_id={'cp': dev}, device_id_type=MESH)

    def partial(val):
        parts = val.reshape(val.shape[0] // 8, 8, n_chan)
        return jnp.sum(parts, axis=0), jnp.sum(parts * parts, axis=0)

    def send_stats(exch, smp, sums):
        row = lax.broadcasted_iota(jnp.int32, (8, n_chan), 0)
        first = jnp.sum(sums[0], axis=0, keepdims=True)
        second = jnp.sum(sums[1], axis=0, keepdims=True)
        both = jnp.where(row == 0, first, jnp.where(row == 1, second, 0.0))
        both = group_total(both, (1, 2, 4, 8))
        lane = lax.broadcasted_iota(jnp.int32, (8, 128), 1)
        packed = both[:, :128]
        for idx in range(1, n_vreg):
            packed = jnp.where((lane & 3) == idx, both[:, idx * 128:(idx + 1) * 128], packed)
        stat_src[exch, smp] = packed
        for dist in range(1, n_dev):
            remote(stat_src.at[exch, smp], stat_rcv.at[exch, smp, dist - 1], st_send.at[exch, smp],
                   st_recv.at[exch, smp], lax.rem(me + dist, n_dev)).start()

    def wait_stats(exch, smp):
        every = stat_rcv.at[exch, smp]
        pltpu.make_async_copy(every, every, st_recv.at[exch, smp]).wait()
        pltpu.make_async_copy(every, every, st_send.at[exch, smp]).wait()

    def affine(exch, smp, norm):
        total = stat_src[exch, smp] + jnp.sum(stat_rcv[exch, smp], axis=0)
        lane = lax.broadcasted_iota(jnp.int32, (8, 128), 1)
        spread = [group_total(jnp.where((lane & 3) == idx, total, 0.0), (1, 2)) for idx in range(n_vreg)]
        full = jnp.concatenate(spread, axis=1)
        mean = full[0:1, :] / count
        inv = lax.rsqrt(full[1:2, :] / count - mean * mean + GN_EPS)
        mul = inv * row_of(GAIN + norm)
        return mul, row_of(SHIFT + norm) - mean * mul

    def halo_copies(exch, smp, buf):
        top = remote(buf.at[smp, pl.ds(0, width)], halo.at[exch, smp, 1], ha_send.at[exch, smp, 0], ha_recv.at[exch, smp, 1], above)
        bottom = remote(buf.at[smp, pl.ds(n_tok - width, width)], halo.at[exch, smp, 0], ha_send.at[exch, smp, 1], ha_recv.at[exch, smp, 0], below)
        return top, bottom

    def send_halo(exch, smp, buf):
        for copy in halo_copies(exch, smp, buf):
            copy.start()

    def wait_halo(exch, smp, buf):
        for copy in halo_copies(exch, smp, buf):
            copy.wait()

    col = lax.broadcasted_iota(jnp.int32, (width, n_chan), 0)
    taps = 3 * n_chan

    def conv_core(rows_out, edge, load, keep_top, keep_bottom, mul, add, conv, res, store):
        def put(row, keep):
            half = 0.5 * (load(row).astype(F32) * mul + add)
            act = half + half * jnp.tanh(half)
            if keep is not None:
                act = jnp.where(keep, act, 0.0)
            left = jnp.where(col == 0, 0.0, pltpu.roll(act, 1, 0))
            right = jnp.where(col == width - 1, 0.0, pltpu.roll(act, width - 1, 0))
            u3[pl.ds(row * width, width), :n_chan] = left.astype(BF16)
            u3[pl.ds(row * width, width), n_chan:2 * n_chan] = act.astype(BF16)
            u3[pl.ds(row * width, width), 2 * n_chan:] = right.astype(BF16)

        def put_row(row, carry):
            put(row, None)
            return carry

        half_rows = rows_out // 2

        def put_top(row, carry):
            put(row, keep_top)
            return carry

        if edge == 1:
            put(0, keep_top)
        else:
            lax.fori_loop(0, edge, put_top, 0)
        lax.fori_loop(edge, half_rows + 2, put_row, 0)
        span = half_rows * width
        bias = row_of(B_CONV + conv)
        sums = [jnp.zeros((8, n_chan), F32)] * 2
        for idx in range(2):
            base = idx * span
            total = bias
            for dy in range(3):
                start = base + dy * width
                total = total + jnp.dot(u3[start:start + span, :], wbuf[conv % 2, dy * taps:(dy + 1) * taps, :], preferred_element_type=F32)
            if idx == 0:
                for row in range(half_rows + 2, rows_out + 2 - edge):
                    put(row, None)
                for row in range(rows_out + 2 - edge, rows_out + 2):
                    put(row, keep_bottom)
            if res is not None:
                total = total + res(base, span).astype(F32)
            rounded = total.astype(BF16)
            store(base, span, rounded)
            sums = [old + new for old, new in zip(sums, partial(rounded.astype(F32)))]
        return sums

    def conv_sample(smp, conv, norm, exch, hexch, src, dst, res):
        wait_stats(exch, smp)
        wait_halo(hexch, smp, src)
        mul, add = affine(exch, smp, norm)

        def load(row):
            if isinstance(row, int) and row == 0:
                return halo[hexch, smp, 0]
            if isinstance(row, int) and row == n_rows + 1:
                return halo[hexch, smp, 1]
            return src[smp, pl.ds((row - 1) * width, width), :]

        def store(base, span, val):
            dst[smp, base:base + span, :] = val

        get = None if res is None else lambda base, span: res[smp, base:base + span, :]
        return conv_core(n_rows, 1, load, me > 0, me < n_dev - 1, mul, add, conv, get, store)

    n_z = lat.shape[2]
    rows = [jnp.concatenate([lat[0, row].astype(F32), lat[1, row].astype(F32)], axis=0) for row in range(n_rows)]
    z_src[0] = rows[0]
    z_src[1] = rows[-1]
    blank = jnp.zeros((n_z, n_chan), F32)
    for smp in range(2):
        pieces = []
        for tap in range(9):
            pair = [blank, blank]
            pair[smp] = w_in[tap].astype(F32)
            pieces += pair
        pieces.append(jnp.zeros((128 - 18 * n_z, n_chan), F32))
        w_first[smp] = jnp.concatenate(pieces, axis=0).astype(BF16)
    pl.semaphore_wait(barrier, n_dev - 1)
    z_copies = (remote(z_src.at[0], z_halo.at[1], z_send.at[0], z_recv.at[1], above),
                remote(z_src.at[1], z_halo.at[0], z_send.at[1], z_recv.at[0], below))
    for copy in z_copies:
        copy.start()
    half_ring = n_dev // 2
    base_dev = me - core + half_ring
    side_dev = base_dev + 4 * core - 2
    far_copies = []
    for smp in range(2):
        far_copies.append(remote(lat.at[smp], z_far.at[1 + core], zf_send.at[smp], zf_recv.at[1 + core], lax.rem(base_dev + smp, n_dev)))
        far_copies.append(remote(lat.at[smp], z_far.at[3 - 3 * core], zf_send.at[2 + smp], zf_recv.at[3 - 3 * core],
                                 lax.rem(side_dev + smp, n_dev)))
    for copy in far_copies:
        copy.start()
    for copy in z_copies:
        copy.wait()
    rows = [jnp.where(me > 0, z_halo[0], 0.0)] + rows + [jnp.where(me < n_dev - 1, z_halo[1], 0.0)]
    lane = lax.broadcasted_iota(jnp.int32, (2 * n_z, width), 1)

    def columns(lines):
        n_out = len(lines) - 2
        for tap in range(9):
            dy, dx = tap // 3, tap % 3
            moved = lines[dy:dy + n_out]
            if dx == 0:
                moved = [jnp.where(lane == 0, 0.0, pltpu.roll(line, 1, 1)) for line in moved]
            if dx == 2:
                moved = [jnp.where(lane == width - 1, 0.0, pltpu.roll(line, width - 1, 1)) for line in moved]
            z_col[tap * 2 * n_z:(tap + 1) * 2 * n_z, :n_out * width] = jnp.concatenate(moved, axis=1)
        z_tok[:n_out * width, :] = jnp.transpose(z_col[:, :n_out * width]).astype(BF16)

    z_col[18 * n_z:, :] = jnp.zeros((128 - 18 * n_z, n_tok), F32)
    columns(rows)

    def first(smp, carry):
        total = jnp.dot(z_tok[...], w_first[smp], preferred_element_type=F32) + row_of(B_IN)
        rounded = total.astype(BF16)
        hbuf[smp] = rounded
        send_halo(0, smp, hbuf)
        send_stats(0, smp, partial(rounded.astype(F32)))
        return carry

    lax.fori_loop(0, 2, first, 0)

    load_att.wait()
    wabuf[1] = jnp.transpose(wabuf[1].astype(F32)).astype(BF16)
    bk_col[...] = jnp.transpose(jnp.broadcast_to(row_of(B_ATT + 1), (128, n_chan)))
    q_len = n_tok // 2

    def clear(blk, carry):
        rows = pl.ds(blk * q_len, q_len)
        mx[rows, :] = jnp.full((q_len, 128), -jnp.inf, F32)
        ls[rows, :] = jnp.zeros((q_len, 128), F32)
        acc[rows, :] = jnp.zeros((q_len, n_chan), F32)
        return carry

    lax.fori_loop(0, 4, clear, 0)

    load_weights(0).wait()

    def stage0(smp, carry):
        sums = conv_sample(smp, 0, 0, 0, 0, hbuf, tbuf, None)
        send_halo(1, smp, tbuf)
        send_stats(1, smp, sums)
        return carry

    lax.fori_loop(0, 2, stage0, 0)
    load_weights(1).wait()

    def forward(src, idx):
        slot = idx + 1 + idx // 5
        return remote(ring.at[src], ring.at[slot], rg_send.at[0, idx], rg_recv.at[slot], ahead)

    def backward(src, idx):
        slot = idx + 9 + idx // 5
        return remote(ring.at[src], ring.at[slot], rg_send.at[1, idx], rg_recv.at[slot], behind)

    def arrived(slot):
        remote(ring.at[slot], ring.at[slot], rg_send.at[0, 0], rg_recv.at[slot], behind).wait_recv()

    def swap():
        return remote(hbuf.at[1 - core], ring.at[8], sw_send, sw_recv, mate)

    def stage1(smp, carry):
        sums = conv_sample(smp, 1, 1, 1, 1, tbuf, hbuf, hbuf)
        send_stats(2, smp, sums)

        @pl.when(smp == 1 - core)
        def _():
            swap().start()

        @pl.when(smp == core)
        def _():
            ring[0] = hbuf[smp]
            forward(0, 0).start()
            backward(0, 1).start()

        return carry

    lax.fori_loop(0, 2, stage1, 0)
    scale = n_chan ** -0.5 * math.log2(math.e)

    def norm_slot(slot):
        nbuf[...] = (ring[slot].astype(F32) * row_of(NORM_ATT) + row_of(NORM_ATT + 1)).astype(BF16)

    def query(slot, carry):
        norm_slot(8 * slot)
        proj = jnp.dot(nbuf[...], wabuf[0], preferred_element_type=F32) + row_of(B_ATT)
        qbuf[pl.ds(slot * n_tok, n_tok), :] = proj.astype(BF16)
        return carry


    def attend(slot):
        norm_slot(slot)
        keys = lax.dot_general(wabuf[1], nbuf[...], (((1,), (1,)), ((), ())), preferred_element_type=F32)
        kt[...] = (keys + bk_col[:, 0:1]).astype(BF16)
        scores = jnp.dot(qbuf[:q_len, :], kt[...], preferred_element_type=F32)
        vals = jnp.dot(nbuf[...], wabuf[2], preferred_element_type=F32) + row_of(B_ATT + 2)
        vbuf[...] = vals.astype(BF16)

        def score(blk):
            return jnp.dot(qbuf[blk * q_len:(blk + 1) * q_len, :], kt[...], preferred_element_type=F32)

        n_part = max(n_tok // 128, 1)
        wide = n_tok // n_part
        for blk in range(4):
            following = score(blk + 1) if blk < 3 else None
            rows = slice(blk * q_len, (blk + 1) * q_len)
            cols = [scores[:, idx * wide:(idx + 1) * wide] for idx in range(n_part)]
            old = mx[rows, :]
            new = jnp.maximum(old, jnp.max(functools.reduce(jnp.maximum, cols), axis=1, keepdims=True) * scale)
            fade = jnp.exp2(old - new)
            prob = [jnp.exp2(col * scale - new[:, :wide]) for col in cols]
            mx[rows, :] = new
            ls[rows, :wide] = ls[rows, :wide] * fade[:, :wide] + functools.reduce(jnp.add, prob)
            prob = jnp.concatenate([col.astype(BF16) for col in prob], axis=1)
            acc[rows, :] = acc[rows, :] * jnp.concatenate([fade] * n_vreg, axis=1) + jnp.dot(prob, vbuf[...], preferred_element_type=F32)
            scores = following

    far = lax.rem(me - core + half_ring, n_dev)
    far_rows = n_rows + 4

    def far_first(part):
        band = far + part
        inside = (band > 0, band < n_dev - 1)

        @pl.when(part == 0)
        def _():
            for slot in range(4):
                remote(lat.at[0], z_far.at[slot], zf_send.at[slot], zf_recv.at[slot], mate).wait()

        blank_z = jnp.zeros((n_z, width), F32)

        def line(slot, row, keep):
            val = z_far[slot, row].astype(F32)
            if keep is not None:
                val = jnp.where(keep, val, 0.0)
            return jnp.concatenate([val, blank_z], axis=0)

        lines = [line(part, n_rows - 3 + row, inside[0]) for row in range(3)]
        lines += [line(part + 1, row, None) for row in range(n_rows)]
        lines += [line(part + 2, row, inside[1]) for row in range(3)]
        half_far = far_rows // 2
        for idx in range(2):
            columns(lines[idx * half_far:(idx + 1) * half_far + 2])
            total = jnp.dot(z_tok[:half_far * width, :], w_first[0], preferred_element_type=F32) + row_of(B_IN)
            far_in[idx * half_far * width:(idx + 1) * half_far * width, :] = total.astype(BF16)
        mul, add = affine(0, core, 0)

        def store(base, span, val):
            far_mid[base:base + span, :] = val

        conv_core(n_rows + 2, 2, lambda row: far_in[pl.ds(row * width, width), :], inside[0], inside[1], mul, add, 0, None, store)

    def far_second(part):
        band = far + part
        mul, add = affine(1, core, 1)

        def store(base, span, val):
            ring[6 + 8 * part, base:base + span, :] = val

        conv_core(n_rows, 1, lambda row: far_mid[pl.ds(row * width, width), :], band > 0, band < n_dev - 1, mul, add, 1,
                  lambda base, span: far_in[base + 2 * width:base + 2 * width + span, :], store)

    def step(idx, carry):
        half = idx // 2
        odd = idx % 2

        @pl.when((idx == 0) | (idx == 4))
        def _():
            far_first(idx // 4)

        @pl.when((idx == 2) | (idx == 8))
        def _():
            far_second(idx // 8)

        @pl.when(idx == 8)
        def _():
            load_weights(2).start()
            load_weights(3).start()

        @pl.when(idx == 0)
        def _():
            swap().wait()
            forward(8, 1).start()
            backward(8, 0).start()
            wait_stats(2, core)
            mul, add = affine(2, core, 2)
            par[NORM_ATT:NORM_ATT + 1, :] = mul
            par[NORM_ATT + 1:NORM_ATT + 2, :] = add
            lax.fori_loop(0, 2, query, 0)

        @pl.when((idx >= 2) & (half != 6))
        def _():
            arrived(half + 8 * odd)

            @pl.when((half <= 4) & (odd == 0))
            def _():
                forward(half, half + 1).start()

            @pl.when((half <= 4) & (odd == 1))
            def _():
                backward(8 + half, half + 1).start()

        attend(half + 8 * odd)
        return carry

    lax.fori_loop(0, n_dev, step, 0)

    def drain(idx, carry):
        forward(0, idx).wait_send()
        backward(0, idx).wait_send()
        return carry

    lax.fori_loop(0, 6, drain, 0)
    wait_stats(2, 1 - core)

    def finish(base, put_out):
        part = q_len // 2

        def one(blk, carry):
            rows = pl.ds(base + blk * part, part)
            total = jnp.sum(ls[rows, :], axis=1, keepdims=True)
            put_out(pl.ds(blk * part, part), (acc[rows, :] / total).astype(BF16))
            return carry

        lax.fori_loop(0, 4, one, 0)

    def to_mate(rows, val):
        vbuf[rows, :] = val

    def to_self(rows, val):
        obuf[0, rows, :] = val

    finish(n_tok, to_mate)
    give = remote(vbuf, obuf.at[1], o_send, o_recv, mate)
    give.start()
    finish(0, to_self)

    def project(side, carry):
        @pl.when(side == 1)
        def _():
            give.wait()

        smp = lax.rem(core + side, 2)
        total = jnp.dot(obuf[side], wabuf[3], preferred_element_type=F32) + row_of(B_ATT + 3)
        rounded = (hbuf[smp].astype(F32) + total).astype(BF16)
        hbuf[smp] = rounded
        send_halo(2, smp, hbuf)
        send_stats(3, smp, partial(rounded.astype(F32)))
        return carry

    lax.fori_loop(0, 2, project, 0)
    load_weights(2).wait()

    def stage2(smp, carry):
        sums = conv_sample(smp, 2, 3, 3, 2, hbuf, tbuf, None)
        send_halo(3, smp, tbuf)
        send_stats(4, smp, sums)
        return carry

    lax.fori_loop(0, 2, stage2, 0)
    load_weights(3).wait()

    def write(smp):
        return pltpu.make_async_copy(tbuf.at[smp], out.at[smp], out_sem.at[smp])

    def stage3(smp, carry):
        conv_sample(smp, 3, 4, 4, 3, tbuf, tbuf, hbuf)
        write(smp).start()
        return carry

    lax.fori_loop(0, 2, stage3, 0)
    write(0).wait()
    write(1).wait()


def decoder(n_dev, lat, w_in, b_in, b_conv, gain, shift, b_att, w_conv, w_att):
    n_rows, n_z, width = lat.shape[1:]
    n_chan = w_in.shape[-1]
    n_tok = n_rows * width
    vmem = pltpu.VMEM
    dma = pltpu.SemaphoreType.DMA
    in_vmem = pl.BlockSpec(memory_space=pltpu.VMEM)
    in_any = pl.BlockSpec(memory_space=pl.ANY)
    scratch = [
        vmem((2, n_tok, n_chan), BF16),
        vmem((2, n_tok, n_chan), BF16),
        vmem((n_tok + 4 * width, 3 * n_chan), BF16),
        vmem((2, 9 * n_chan, n_chan), BF16),
        vmem((4, n_chan, n_chan), BF16),
        vmem((4, 2, 2, width, n_chan), BF16),
        vmem((5, 2, 8, 128), F32),
        vmem((5, 2, n_dev - 1, 8, 128), F32),
        vmem((n_dev, n_tok, n_chan), BF16),
        vmem((2 * n_tok, n_chan), BF16),
        vmem((2 * n_tok, n_chan), F32),
        vmem((2 * n_tok, 128), F32),
        vmem((2 * n_tok, 128), F32),
        vmem((n_tok, n_chan), BF16),
        vmem((n_chan, n_tok), BF16),
        vmem((n_tok, n_chan), BF16),
        vmem((2, n_tok, n_chan), BF16),
        vmem((N_PAR, n_chan), F32),
        vmem((n_chan, 128), F32),
        vmem((2, 128, n_chan), BF16),
        vmem((2, 2 * n_z, width), F32),
        vmem((2, 2 * n_z, width), F32),
        vmem((128, n_tok), F32),
        vmem((n_tok, 128), BF16),
        vmem((4, n_rows, n_z, width), BF16),
        vmem((n_tok + 4 * width, n_chan), BF16),
        vmem((n_tok + 2 * width, n_chan), BF16),
        dma((2,)), dma, dma((5, 2)), dma((5, 2)), dma((4, 2, 2)), dma((4, 2, 2)), dma((2, 6)), dma((n_dev,)),
        dma, dma, dma, dma, dma((2,)), dma((2,)), dma((2,)), dma((4,)), dma((4,)),
    ]
    return pl.pallas_call(
        functools.partial(body, (n_dev, n_rows, width, n_chan)),
        out_shape=jax.ShapeDtypeStruct((2, n_tok, n_chan), BF16),
        in_specs=[in_vmem] * 7 + [in_any] * 2,
        out_specs=in_any,
        scratch_shapes=scratch,
        compiler_params=pltpu.CompilerParams(collective_id=0, has_side_effects=True, vmem_limit_bytes=67043328),
    )(lat, w_in, b_in, b_conv, gain, shift, b_att, w_conv, w_att)


def solution(mesh):
    n_dev = mesh.shape['cp']

    def local_fn(latents, w_in, b_in, w_conv, b_conv, gn_scale, gn_shift, w_attn, b_attn):
        n_batch, n_rows, width, n_z = latents.shape
        n_chan = w_in.shape[-1]
        out = decoder(n_dev, latents.transpose(0, 1, 3, 2), w_in.reshape(9, n_z, n_chan), b_in, b_conv, gn_scale,
                      gn_shift, b_attn, w_conv.reshape(4, 9 * n_chan, n_chan), w_attn)
        return out.reshape(n_batch, n_rows, width, n_chan)

    band_spec = P('dp', 'cp')
    whole_spec = P()
    return jax.shard_map(local_fn, mesh=mesh, in_specs=(band_spec,) + (whole_spec,) * 8, out_specs=band_spec, check_vma=False)
```

```python
import functools
import math

import jax
import jax.numpy as jnp
from jax import lax
from jax.experimental import pallas as pl
from jax.experimental.pallas import tpu as pltpu
from jax.sharding import PartitionSpec as P

F32 = jnp.float32
BF16 = jnp.bfloat16
GROUPS = 32
GN_EPS = 1e-6
MESH = pl.DeviceIdType.MESH
B_IN, B_CONV, GAIN, SHIFT, B_ATT, NORM_ATT, N_PAR = 0, 1, 5, 10, 15, 19, 24


def group_total(x_val, steps):
    lane = lax.broadcasted_iota(jnp.int32, x_val.shape, 1)
    width = x_val.shape[1]
    for step in steps:
        above = pltpu.roll(x_val, width - step, 1)
        below = pltpu.roll(x_val, step, 1)
        x_val = x_val + jnp.where((lane & step) == 0, above, below)
    return x_val


def body(cfg, lat, w_in, b_in, b_conv, gain, shift, b_att, w_conv, w_att, out, hbuf, tbuf, u3, wbuf, wabuf, halo, stat_src, stat_rcv,
         ring, qbuf, acc, mx, ls, nbuf, kt, vbuf, obuf, par, bk_col, w_first, z_src, z_halo, z_col, z_tok, z_far, far_in, far_mid,
         w_sem, wa_sem, st_send, st_recv, ha_send, ha_recv, rg_send, rg_recv, sw_send, sw_recv, o_send, o_recv, out_sem, z_send, z_recv, zf_send, zf_recv):
    n_dev, n_rows, width, n_chan = cfg
    n_tok = n_rows * width
    lanes = n_chan // GROUPS
    n_vreg = n_chan // 128
    count = n_dev * n_tok * lanes
    me = lax.axis_index('cp')
    core = lax.rem(me, 2)
    mate = me + 1 - 2 * core
    ahead = lax.rem(me + 2, n_dev)
    behind = lax.rem(me + n_dev - 2, n_dev)
    below = lax.rem(me + 1, n_dev)
    above = lax.rem(me + n_dev - 1, n_dev)

    barrier = pltpu.get_barrier_semaphore()
    for dist in range(1, n_dev):
        pl.semaphore_signal(barrier, inc=1, device_id={'cp': lax.rem(me + dist, n_dev)}, device_id_type=MESH)

    def load_weights(idx):
        return pltpu.make_async_copy(w_conv.at[idx], wbuf.at[idx % 2], w_sem.at[idx % 2])

    load_weights(0).start()
    load_weights(1).start()
    load_att = pltpu.make_async_copy(w_att, wabuf, wa_sem)
    load_att.start()

    par[...] = jnp.zeros(par.shape, F32)
    par[B_IN:B_IN + 1, :] = b_in[...].astype(F32).reshape(1, n_chan)
    par[B_CONV:B_CONV + 4, :] = b_conv[...].astype(F32)
    par[GAIN:GAIN + 5, :] = gain[...].astype(F32)
    par[SHIFT:SHIFT + 5, :] = shift[...].astype(F32)
    par[B_ATT:B_ATT + 4, :] = b_att[...].astype(F32)

    def row_of(idx):
        return par[pl.ds(idx, 1), :]

    def remote(src, dst, send_sem, recv_sem, dev):
        return pltpu.make_async_remote_copy(src_ref=src, dst_ref=dst, send_sem=send_sem, recv_sem=recv_sem,
                                            device_id={'cp': dev}, device_id_type=MESH)

    def partial(val):
        parts = val.reshape(val.shape[0] // 8, 8, n_chan)
        return jnp.sum(parts, axis=0), jnp.sum(parts * parts, axis=0)

    def send_stats(exch, smp, sums):
        row = lax.broadcasted_iota(jnp.int32, (8, n_chan), 0)
        first = jnp.sum(sums[0], axis=0, keepdims=True)
        second = jnp.sum(sums[1], axis=0, keepdims=True)
        both = jnp.where(row == 0, first, jnp.where(row == 1, second, 0.0))
        both = group_total(both, (1, 2, 4, 8))
        lane = lax.broadcasted_iota(jnp.int32, (8, 128), 1)
        packed = both[:, :128]
        for idx in range(1, n_vreg):
            packed = jnp.where((lane & 3) == idx, both[:, idx * 128:(idx + 1) * 128], packed)
        stat_src[exch, smp] = packed
        for dist in range(1, n_dev):
            remote(stat_src.at[exch, smp], stat_rcv.at[exch, smp, dist - 1], st_send.at[exch, smp],
                   st_recv.at[exch, smp], lax.rem(me + dist, n_dev)).start()

    def wait_stats(exch, smp):
        every = stat_rcv.at[exch, smp]
        pltpu.make_async_copy(every, every, st_recv.at[exch, smp]).wait()
        pltpu.make_async_copy(every, every, st_send.at[exch, smp]).wait()

    def affine(exch, smp, norm):
        total = stat_src[exch, smp] + jnp.sum(stat_rcv[exch, smp], axis=0)
        lane = lax.broadcasted_iota(jnp.int32, (8, 128), 1)
        spread = [group_total(jnp.where((lane & 3) == idx, total, 0.0), (1, 2)) for idx in range(n_vreg)]
        full = jnp.concatenate(spread, axis=1)
        mean = full[0:1, :] / count
        inv = lax.rsqrt(full[1:2, :] / count - mean * mean + GN_EPS)
        mul = inv * row_of(GAIN + norm)
        return mul, row_of(SHIFT + norm) - mean * mul

    def halo_copies(exch, smp, buf):
        top = remote(buf.at[smp, pl.ds(0, width)], halo.at[exch, smp, 1], ha_send.at[exch, smp, 0], ha_recv.at[exch, smp, 1], above)
        bottom = remote(buf.at[smp, pl.ds(n_tok - width, width)], halo.at[exch, smp, 0], ha_send.at[exch, smp, 1], ha_recv.at[exch, smp, 0], below)
        return top, bottom

    def send_halo(exch, smp, buf):
        for copy in halo_copies(exch, smp, buf):
            copy.start()

    def wait_halo(exch, smp, buf):
        for copy in halo_copies(exch, smp, buf):
            copy.wait()

    col = lax.broadcasted_iota(jnp.int32, (width, n_chan), 0)
    taps = 3 * n_chan

    def conv_core(rows_out, edge, load, keep_top, keep_bottom, mul, add, conv, res, store):
        def put(row, keep):
            half = 0.5 * (load(row).astype(F32) * mul + add)
            act = half + half * jnp.tanh(half)
            if keep is not None:
                act = jnp.where(keep, act, 0.0)
            left = jnp.where(col == 0, 0.0, pltpu.roll(act, 1, 0))
            right = jnp.where(col == width - 1, 0.0, pltpu.roll(act, width - 1, 0))
            u3[pl.ds(row * width, width), :n_chan] = left.astype(BF16)
            u3[pl.ds(row * width, width), n_chan:2 * n_chan] = act.astype(BF16)
            u3[pl.ds(row * width, width), 2 * n_chan:] = right.astype(BF16)

        def put_row(row, carry):
            put(row, None)
            return carry

        half_rows = rows_out // 2

        def put_top(row, carry):
            put(row, keep_top)
            return carry

        if edge == 1:
            put(0, keep_top)
        else:
            lax.fori_loop(0, edge, put_top, 0)
        lax.fori_loop(edge, half_rows + 2, put_row, 0)
        span = half_rows * width
        bias = row_of(B_CONV + conv)
        sums = [jnp.zeros((8, n_chan), F32)] * 2
        for idx in range(2):
            base = idx * span
            total = bias
            for dy in range(3):
                start = base + dy * width
                total = total + jnp.dot(u3[start:start + span, :], wbuf[conv % 2, dy * taps:(dy + 1) * taps, :], preferred_element_type=F32)
            if idx == 0:
                for row in range(half_rows + 2, rows_out + 2 - edge):
                    put(row, None)
                for row in range(rows_out + 2 - edge, rows_out + 2):
                    put(row, keep_bottom)
            if res is not None:
                total = total + res(base, span).astype(F32)
            rounded = total.astype(BF16)
            store(base, span, rounded)
            sums = [old + new for old, new in zip(sums, partial(rounded.astype(F32)))]
        return sums

    def conv_sample(smp, conv, norm, exch, hexch, src, dst, res):
        wait_stats(exch, smp)
        wait_halo(hexch, smp, src)
        mul, add = affine(exch, smp, norm)

        def load(row):
            if isinstance(row, int) and row == 0:
                return halo[hexch, smp, 0]
            if isinstance(row, int) and row == n_rows + 1:
                return halo[hexch, smp, 1]
            return src[smp, pl.ds((row - 1) * width, width), :]

        def store(base, span, val):
            dst[smp, base:base + span, :] = val

        get = None if res is None else lambda base, span: res[smp, base:base + span, :]
        return conv_core(n_rows, 1, load, me > 0, me < n_dev - 1, mul, add, conv, get, store)

    n_z = lat.shape[2]
    rows = [jnp.concatenate([lat[0, row].astype(F32), lat[1, row].astype(F32)], axis=0) for row in range(n_rows)]
    z_src[0] = rows[0]
    z_src[1] = rows[-1]
    blank = jnp.zeros((n_z, n_chan), F32)
    for smp in range(2):
        pieces = []
        for tap in range(9):
            pair = [blank, blank]
            pair[smp] = w_in[tap].astype(F32)
            pieces += pair
        pieces.append(jnp.zeros((128 - 18 * n_z, n_chan), F32))
        w_first[smp] = jnp.concatenate(pieces, axis=0).astype(BF16)
    pl.semaphore_wait(barrier, n_dev - 1)
    z_copies = (remote(z_src.at[0], z_halo.at[1], z_send.at[0], z_recv.at[1], above),
                remote(z_src.at[1], z_halo.at[0], z_send.at[1], z_recv.at[0], below))
    for copy in z_copies:
        copy.start()
    half_ring = n_dev // 2
    base_dev = me - core + half_ring
    side_dev = base_dev + 4 * core - 2
    far_copies = []
    for smp in range(2):
        far_copies.append(remote(lat.at[smp], z_far.at[1 + core], zf_send.at[smp], zf_recv.at[1 + core], lax.rem(base_dev + smp, n_dev)))
        far_copies.append(remote(lat.at[smp], z_far.at[3 - 3 * core], zf_send.at[2 + smp], zf_recv.at[3 - 3 * core],
                                 lax.rem(side_dev + smp, n_dev)))
    for copy in far_copies:
        copy.start()
    for copy in z_copies:
        copy.wait()
    rows = [jnp.where(me > 0, z_halo[0], 0.0)] + rows + [jnp.where(me < n_dev - 1, z_halo[1], 0.0)]
    lane = lax.broadcasted_iota(jnp.int32, (2 * n_z, width), 1)

    def columns(lines):
        n_out = len(lines) - 2
        for tap in range(9):
            dy, dx = tap // 3, tap % 3
            moved = lines[dy:dy + n_out]
            if dx == 0:
                moved = [jnp.where(lane == 0, 0.0, pltpu.roll(line, 1, 1)) for line in moved]
            if dx == 2:
                moved = [jnp.where(lane == width - 1, 0.0, pltpu.roll(line, width - 1, 1)) for line in moved]
            z_col[tap * 2 * n_z:(tap + 1) * 2 * n_z, :n_out * width] = jnp.concatenate(moved, axis=1)
        z_tok[:n_out * width, :] = jnp.transpose(z_col[:, :n_out * width]).astype(BF16)

    z_col[18 * n_z:, :] = jnp.zeros((128 - 18 * n_z, n_tok), F32)
    columns(rows)

    def first(smp, carry):
        total = jnp.dot(z_tok[...], w_first[smp], preferred_element_type=F32) + row_of(B_IN)
        rounded = total.astype(BF16)
        hbuf[smp] = rounded
        send_halo(0, smp, hbuf)
        send_stats(0, smp, partial(rounded.astype(F32)))
        return carry

    lax.fori_loop(0, 2, first, 0)

    load_att.wait()
    wabuf[1] = jnp.transpose(wabuf[1].astype(F32)).astype(BF16)
    bk_col[...] = jnp.transpose(jnp.broadcast_to(row_of(B_ATT + 1), (128, n_chan)))
    q_len = n_tok // 2

    def clear(blk, carry):
        rows = pl.ds(blk * q_len, q_len)
        mx[rows, :] = jnp.full((q_len, 128), -jnp.inf, F32)
        ls[rows, :] = jnp.zeros((q_len, 128), F32)
        acc[rows, :] = jnp.zeros((q_len, n_chan), F32)
        return carry

    lax.fori_loop(0, 4, clear, 0)

    load_weights(0).wait()

    def stage0(smp, carry):
        sums = conv_sample(smp, 0, 0, 0, 0, hbuf, tbuf, None)
        send_halo(1, smp, tbuf)
        send_stats(1, smp, sums)
        return carry

    lax.fori_loop(0, 2, stage0, 0)
    load_weights(1).wait()

    def forward(src, idx):
        slot = idx + 1 + idx // 5
        return remote(ring.at[src], ring.at[slot], rg_send.at[0, idx], rg_recv.at[slot], ahead)

    def backward(src, idx):
        slot = idx + 9 + idx // 5
        return remote(ring.at[src], ring.at[slot], rg_send.at[1, idx], rg_recv.at[slot], behind)

    def arrived(slot):
        remote(ring.at[slot], ring.at[slot], rg_send.at[0, 0], rg_recv.at[slot], behind).wait_recv()

    def swap():
        return remote(hbuf.at[1 - core], ring.at[8], sw_send, sw_recv, mate)

    def stage1(smp, carry):
        sums = conv_sample(smp, 1, 1, 1, 1, tbuf, hbuf, hbuf)
        send_stats(2, smp, sums)

        @pl.when(smp == 1 - core)
        def _():
            swap().start()

        @pl.when(smp == core)
        def _():
            ring[0] = hbuf[smp]
            forward(0, 0).start()
            backward(0, 0).start()

        return carry

    lax.fori_loop(0, 2, stage1, 0)
    scale = n_chan ** -0.5 * math.log2(math.e)

    def norm_slot(slot):
        nbuf[...] = (ring[slot].astype(F32) * row_of(NORM_ATT) + row_of(NORM_ATT + 1)).astype(BF16)

    def query(slot, carry):
        norm_slot(8 * slot)
        proj = jnp.dot(nbuf[...], wabuf[0], preferred_element_type=F32) + row_of(B_ATT)
        qbuf[pl.ds(slot * n_tok, n_tok), :] = proj.astype(BF16)
        return carry


    def attend(slot):
        norm_slot(slot)
        keys = lax.dot_general(wabuf[1], nbuf[...], (((1,), (1,)), ((), ())), preferred_element_type=F32)
        kt[...] = (keys + bk_col[:, 0:1]).astype(BF16)
        scores = jnp.dot(qbuf[:q_len, :], kt[...], preferred_element_type=F32)
        vals = jnp.dot(nbuf[...], wabuf[2], preferred_element_type=F32) + row_of(B_ATT + 2)
        vbuf[...] = vals.astype(BF16)

        def score(blk):
            return jnp.dot(qbuf[blk * q_len:(blk + 1) * q_len, :], kt[...], preferred_element_type=F32)

        n_part = max(n_tok // 128, 1)
        wide = n_tok // n_part
        for blk in range(4):
            following = score(blk + 1) if blk < 3 else None
            rows = slice(blk * q_len, (blk + 1) * q_len)
            cols = [scores[:, idx * wide:(idx + 1) * wide] for idx in range(n_part)]
            old = mx[rows, :]
            new = jnp.maximum(old, jnp.max(functools.reduce(jnp.maximum, cols), axis=1, keepdims=True) * scale)
            fade = jnp.exp2(old - new)
            prob = [jnp.exp2(col * scale - new[:, :wide]) for col in cols]
            mx[rows, :] = new
            ls[rows, :wide] = ls[rows, :wide] * fade[:, :wide] + functools.reduce(jnp.add, prob)
            prob = jnp.concatenate([col.astype(BF16) for col in prob], axis=1)
            acc[rows, :] = acc[rows, :] * jnp.concatenate([fade] * n_vreg, axis=1) + jnp.dot(prob, vbuf[...], preferred_element_type=F32)
            scores = following

    far = lax.rem(me - core + half_ring, n_dev)
    far_rows = n_rows + 4

    def far_first(part):
        band = far + part
        inside = (band > 0, band < n_dev - 1)

        @pl.when(part == 0)
        def _():
            for slot in range(4):
                remote(lat.at[0], z_far.at[slot], zf_send.at[slot], zf_recv.at[slot], mate).wait()

        blank_z = jnp.zeros((n_z, width), F32)

        def line(slot, row, keep):
            val = z_far[slot, row].astype(F32)
            if keep is not None:
                val = jnp.where(keep, val, 0.0)
            return jnp.concatenate([val, blank_z], axis=0)

        lines = [line(part, n_rows - 3 + row, inside[0]) for row in range(3)]
        lines += [line(part + 1, row, None) for row in range(n_rows)]
        lines += [line(part + 2, row, inside[1]) for row in range(3)]
        half_far = far_rows // 2
        for idx in range(2):
            columns(lines[idx * half_far:(idx + 1) * half_far + 2])
            total = jnp.dot(z_tok[:half_far * width, :], w_first[0], preferred_element_type=F32) + row_of(B_IN)
            far_in[idx * half_far * width:(idx + 1) * half_far * width, :] = total.astype(BF16)
        mul, add = affine(0, core, 0)

        def store(base, span, val):
            far_mid[base:base + span, :] = val

        conv_core(n_rows + 2, 2, lambda row: far_in[pl.ds(row * width, width), :], inside[0], inside[1], mul, add, 0, None, store)

    def far_second(part):
        band = far + part
        mul, add = affine(1, core, 1)

        def store(base, span, val):
            ring[6 + 8 * part, base:base + span, :] = val

        conv_core(n_rows, 1, lambda row: far_mid[pl.ds(row * width, width), :], band > 0, band < n_dev - 1, mul, add, 1,
                  lambda base, span: far_in[base + 2 * width:base + 2 * width + span, :], store)

    def step(idx, carry):
        half = idx // 2
        odd = idx % 2

        @pl.when((idx == 0) | (idx == 4))
        def _():
            far_first(idx // 4)

        @pl.when((idx == 2) | (idx == 8))
        def _():
            far_second(idx // 8)

        @pl.when(idx == 8)
        def _():
            load_weights(2).start()
            load_weights(3).start()

        @pl.when(idx == 0)
        def _():
            swap().wait()
            forward(8, 1).start()
            backward(8, 1).start()
            wait_stats(2, core)
            mul, add = affine(2, core, 2)
            par[NORM_ATT:NORM_ATT + 1, :] = mul
            par[NORM_ATT + 1:NORM_ATT + 2, :] = add
            lax.fori_loop(0, 2, query, 0)

        @pl.when((idx >= 2) & (half != 6))
        def _():
            arrived(half + 8 * odd)

            @pl.when((half <= 4) & (odd == 0))
            def _():
                forward(half, half + 1).start()

            @pl.when((half <= 4) & (odd == 1))
            def _():
                backward(8 + half, half + 1).start()

        attend(half + 8 * odd)
        return carry

    lax.fori_loop(0, n_dev, step, 0)

    def drain(idx, carry):
        forward(0, idx).wait_send()
        backward(0, idx).wait_send()
        return carry

    lax.fori_loop(0, 6, drain, 0)
    wait_stats(2, 1 - core)

    def finish(base, put_out):
        part = q_len // 2

        def one(blk, carry):
            rows = pl.ds(base + blk * part, part)
            total = jnp.sum(ls[rows, :], axis=1, keepdims=True)
            put_out(pl.ds(blk * part, part), (acc[rows, :] / total).astype(BF16))
            return carry

        lax.fori_loop(0, 4, one, 0)

    def to_mate(rows, val):
        vbuf[rows, :] = val

    def to_self(rows, val):
        obuf[0, rows, :] = val

    finish(n_tok, to_mate)
    give = remote(vbuf, obuf.at[1], o_send, o_recv, mate)
    give.start()
    finish(0, to_self)

    def project(side, carry):
        @pl.when(side == 1)
        def _():
            give.wait()

        smp = lax.rem(core + side, 2)
        total = jnp.dot(obuf[side], wabuf[3], preferred_element_type=F32) + row_of(B_ATT + 3)
        rounded = (hbuf[smp].astype(F32) + total).astype(BF16)
        hbuf[smp] = rounded
        send_halo(2, smp, hbuf)
        send_stats(3, smp, partial(rounded.astype(F32)))
        return carry

    lax.fori_loop(0, 2, project, 0)
    load_weights(2).wait()

    def stage2(smp, carry):
        sums = conv_sample(smp, 2, 3, 3, 2, hbuf, tbuf, None)
        send_halo(3, smp, tbuf)
        send_stats(4, smp, sums)
        return carry

    lax.fori_loop(0, 2, stage2, 0)
    load_weights(3).wait()

    def write(smp):
        return pltpu.make_async_copy(tbuf.at[smp], out.at[smp], out_sem.at[smp])

    def stage3(smp, carry):
        conv_sample(smp, 3, 4, 4, 3, tbuf, tbuf, hbuf)
        write(smp).start()
        return carry

    lax.fori_loop(0, 2, stage3, 0)
    write(0).wait()
    write(1).wait()


def decoder(n_dev, lat, w_in, b_in, b_conv, gain, shift, b_att, w_conv, w_att):
    n_rows, n_z, width = lat.shape[1:]
    n_chan = w_in.shape[-1]
    n_tok = n_rows * width
    vmem = pltpu.VMEM
    dma = pltpu.SemaphoreType.DMA
    in_vmem = pl.BlockSpec(memory_space=pltpu.VMEM)
    in_any = pl.BlockSpec(memory_space=pl.ANY)
    scratch = [
        vmem((2, n_tok, n_chan), BF16),
        vmem((2, n_tok, n_chan), BF16),
        vmem((n_tok + 4 * width, 3 * n_chan), BF16),
        vmem((2, 9 * n_chan, n_chan), BF16),
        vmem((4, n_chan, n_chan), BF16),
        vmem((4, 2, 2, width, n_chan), BF16),
        vmem((5, 2, 8, 128), F32),
        vmem((5, 2, n_dev - 1, 8, 128), F32),
        vmem((n_dev, n_tok, n_chan), BF16),
        vmem((2 * n_tok, n_chan), BF16),
        vmem((2 * n_tok, n_chan), F32),
        vmem((2 * n_tok, 128), F32),
        vmem((2 * n_tok, 128), F32),
        vmem((n_tok, n_chan), BF16),
        vmem((n_chan, n_tok), BF16),
        vmem((n_tok, n_chan), BF16),
        vmem((2, n_tok, n_chan), BF16),
        vmem((N_PAR, n_chan), F32),
        vmem((n_chan, 128), F32),
        vmem((2, 128, n_chan), BF16),
        vmem((2, 2 * n_z, width), F32),
        vmem((2, 2 * n_z, width), F32),
        vmem((128, n_tok), F32),
        vmem((n_tok, 128), BF16),
        vmem((4, n_rows, n_z, width), BF16),
        vmem((n_tok + 4 * width, n_chan), BF16),
        vmem((n_tok + 2 * width, n_chan), BF16),
        dma((2,)), dma, dma((5, 2)), dma((5, 2)), dma((4, 2, 2)), dma((4, 2, 2)), dma((2, 6)), dma((n_dev,)),
        dma, dma, dma, dma, dma((2,)), dma((2,)), dma((2,)), dma((4,)), dma((4,)),
    ]
    return pl.pallas_call(
        functools.partial(body, (n_dev, n_rows, width, n_chan)),
        out_shape=jax.ShapeDtypeStruct((2, n_tok, n_chan), BF16),
        in_specs=[in_vmem] * 7 + [in_any] * 2,
        out_specs=in_any,
        scratch_shapes=scratch,
        compiler_params=pltpu.CompilerParams(collective_id=0, has_side_effects=True, vmem_limit_bytes=67043328),
    )(lat, w_in, b_in, b_conv, gain, shift, b_att, w_conv, w_att)


def solution(mesh):
    n_dev = mesh.shape['cp']

    def local_fn(latents, w_in, b_in, w_conv, b_conv, gn_scale, gn_shift, w_attn, b_attn):
        n_batch, n_rows, width, n_z = latents.shape
        n_chan = w_in.shape[-1]
        out = decoder(n_dev, latents.transpose(0, 1, 3, 2), w_in.reshape(9, n_z, n_chan), b_in, b_conv, gn_scale,
                      gn_shift, b_attn, w_conv.reshape(4, 9 * n_chan, n_chan), w_attn)
        return out.reshape(n_batch, n_rows, width, n_chan)

    band_spec = P('dp', 'cp')
    whole_spec = P()
    return jax.shard_map(local_fn, mesh=mesh, in_specs=(band_spec,) + (whole_spec,) * 8, out_specs=band_spec, check_vma=False)
```
